8 devices in a mesh: batch: 1 (over z), seq_hi: 2 (over y), seq: 4 (over x, core).
Axes of the slice: x: 2, y: 2, z: 1, core: 2. Of those that a mesh axis runs over, the one named last changes fastest.
Arguments:
- x_seq: bfloat16 [24, 1536, 128], P('batch', ('seq_hi', 'seq'))
- w_f0: bfloat16 [2, 10, 128, 128], replicated
- w_f1: bfloat16 [2, 10, 128, 128], replicated
- w_g0: bfloat16 [2, 10, 128, 128], replicated
- w_g1: bfloat16 [2, 10, 128, 128], replicated
- w_res: bfloat16 [2, 10, 128, 128], replicated
- w_skip: bfloat16 [2, 10, 128, 128], replicated
Outputs:
- output 1: float32 [24, 1536, 128], P('batch', ('seq_hi', 'seq'))
- output 2: float32 [24, 1536, 128], P('batch', ('seq_hi', 'seq'))
All inputs are finite; a program needn't handle non-finite values.
Results may differ from the reference program's by a relative error of at most 0.00640755.
Values are sent between devices in bfloat16 or wider.
A program may use at most 1 GiB of HBM per device.

```python
import jax
import jax.numpy as jnp
from jax import lax

GROUP_SEQS = 24
SEQ_LEN = 1536
CHANNELS = 128
SKIP_CH = 128
DIL_CYCLE = 10
REPEATS = 2


def setup_inputs(seed: int = 0, part: int = 0) -> dict:
    keys = jax.random.split(jax.random.key(seed), 7)
    square = (REPEATS, DIL_CYCLE, CHANNELS, CHANNELS)
    tap_scale = (2 * CHANNELS) ** -0.5
    x_seq = jax.random.normal(jax.random.fold_in(keys[0], part), (GROUP_SEQS, SEQ_LEN, CHANNELS), jnp.float32)
    w_f0 = jax.random.normal(keys[1], square, jnp.float32) * tap_scale
    w_f1 = jax.random.normal(keys[2], square, jnp.float32) * tap_scale
    w_g0 = jax.random.normal(keys[3], square, jnp.float32) * tap_scale
    w_g1 = jax.random.normal(keys[4], square, jnp.float32) * tap_scale
    w_res = jax.random.normal(keys[5], square, jnp.float32) * (0.5 * CHANNELS ** -0.5)
    w_skip = jax.random.normal(keys[6], (REPEATS, DIL_CYCLE, CHANNELS, SKIP_CH), jnp.float32) * CHANNELS ** -0.5
    return {
        "x_seq": x_seq.astype(jnp.bfloat16),
        "w_f0": w_f0.astype(jnp.bfloat16),
        "w_f1": w_f1.astype(jnp.bfloat16),
        "w_g0": w_g0.astype(jnp.bfloat16),
        "w_g1": w_g1.astype(jnp.bfloat16),
        "w_res": w_res.astype(jnp.bfloat16),
        "w_skip": w_skip.astype(jnp.bfloat16),
    }


def mat_mul(left, right):
    return jnp.dot(left, right, preferred_element_type=jnp.float32)


def reference(x_seq, w_f0, w_f1, w_g0, w_g1, w_res, w_skip):
    def one_sequence(seq_in):
        residual = seq_in.astype(jnp.float32)
        skip_acc = jnp.zeros((SEQ_LEN, SKIP_CH), jnp.float32)
        for rep_idx in range(REPEATS):
            for cyc_idx in range(DIL_CYCLE):
                dilation = 2 ** cyc_idx
                current = residual.astype(jnp.bfloat16)
                delayed = jnp.pad(current[:SEQ_LEN - dilation], ((dilation, 0), (0, 0)))
                filter_pre = mat_mul(current, w_f1[rep_idx, cyc_idx]) + mat_mul(delayed, w_f0[rep_idx, cyc_idx])
                gate_pre = mat_mul(current, w_g1[rep_idx, cyc_idx]) + mat_mul(delayed, w_g0[rep_idx, cyc_idx])
                activated = (jnp.tanh(filter_pre) * jax.nn.sigmoid(gate_pre)).astype(jnp.bfloat16)
                residual = residual + mat_mul(activated, w_res[rep_idx, cyc_idx])
                skip_acc = skip_acc + mat_mul(activated, w_skip[rep_idx, cyc_idx])
        return residual, skip_acc
    h_out, skip_out = lax.map(one_sequence, x_seq)
    return h_out, skip_out
```

```python
import functools

import jax
import jax.numpy as jnp
from jax import lax
from jax.experimental import pallas as pl
from jax.experimental.pallas import tpu as pltpu
from jax.sharding import PartitionSpec as P

MESH = pl.DeviceIdType.MESH
SEQ_AXES = ("seq_hi", "seq")
N_DEV = 8
LAG = 2
F32 = jnp.float32
BF16 = jnp.bfloat16


def kernel(n_layers, n_cyc, blk, pad, x_ref, wf0, wf1, wg0, wg1, wr, ws, h_out, s_out,
           xbuf, wg_v, wo_v, ha0, hb0, ha1, hb1, ha2, hb2, hout_v, skip_v,
           w_sem, x_send, x_recv, o_send, h_recv, s_recv):
    hi, lo = lax.axis_index("seq_hi"), lax.axis_index("seq")
    me = hi * 4 + lo
    role = me // 2
    chan = x_ref.shape[-1]

    def dev(index):
        return {"seq_hi": index // 4, "seq": index % 4}

    w_copies = [
        pltpu.make_async_copy(wf1, wg_v.at[:, pl.ds(0, chan), pl.ds(0, chan)], w_sem.at[0]),
        pltpu.make_async_copy(wg1, wg_v.at[:, pl.ds(0, chan), pl.ds(chan, chan)], w_sem.at[1]),
        pltpu.make_async_copy(wf0, wg_v.at[:, pl.ds(chan, chan), pl.ds(0, chan)], w_sem.at[2]),
        pltpu.make_async_copy(wg0, wg_v.at[:, pl.ds(chan, chan), pl.ds(chan, chan)], w_sem.at[3]),
        pltpu.make_async_copy(wr, wo_v.at[:, :, pl.ds(0, chan)], w_sem.at[4]),
        pltpu.make_async_copy(ws, wo_v.at[:, :, pl.ds(chan, chan)], w_sem.at[5]),
    ]
    for copy in w_copies:
        copy.start()

    barrier = pltpu.get_barrier_semaphore()
    for other in range(N_DEV):
        @pl.when(me != other)
        def _():
            pl.semaphore_signal(barrier, inc=1, device_id=dev(other), device_id_type=MESH)
    pl.semaphore_wait(barrier, N_DEV - 1)

    def x_copies(act):
        def one(seq, target, q, unit):
            @pl.when(me == target)
            def _():
                act(pltpu.make_async_copy(x_ref.at[seq], xbuf.at[q, unit], x_recv.at[q]), True)

            @pl.when(me != target)
            def _():
                act(pltpu.make_async_remote_copy(
                    src_ref=x_ref.at[seq], dst_ref=xbuf.at[q, unit], send_sem=x_send, recv_sem=x_recv.at[q],
                    device_id=dev(target), device_id_type=MESH), False)

        for q in range(4):
            for target in range(2):
                if q < 2:
                    @pl.when(me < 4)
                    def _():
                        for half in range(2):
                            one(8 + 4 * target + 2 * q + half, target, q, half * 4 + me)
                else:
                    @pl.when(me < 2)
                    def _():
                        for part in range(4):
                            one(16 * target + 4 * (q - 2) + part, target, q, part * 2 + me)
            for target in range(2, N_DEV):
                one(4 * (target - 2) + q, target, q, me)

    x_copies(lambda copy, local: copy.start())

    def zero_pads(bufs, cps):
        for buf in bufs:
            for first in range(0, 8, cps):
                buf[pl.ds(first // cps * (pad + cps * blk), pad), :] = jnp.zeros((pad, chan), F32)

    @pl.when(role == 0)
    def _():
        zero_pads((ha1, hb1), 4)
        zero_pads((ha2, hb2), 2)

    @pl.when(role != 0)
    def _():
        zero_pads((ha0, hb0), 8)

    for copy in w_copies:
        copy.wait()

    def halve(l, carry):
        wg_v[l, :, pl.ds(chan, chan)] = wg_v[l, :, pl.ds(chan, chan)] * BF16(0.5)
        wo_v[l] = wo_v[l] * BF16(0.5)
        return carry

    lax.fori_loop(0, n_layers, halve, 0)

    def out_copies(act, q, unit, seq, target):
        for src, dst, recv in ((hout_v, h_out, h_recv), (skip_v, s_out, s_recv)):
            @pl.when(me == target)
            def _():
                act(pltpu.make_async_copy(src.at[q, unit], dst.at[seq], recv), True)

            @pl.when(me != target)
            def _():
                act(pltpu.make_async_remote_copy(
                    src_ref=src.at[q, unit], dst_ref=dst.at[seq], send_sem=o_send, recv_sem=recv,
                    device_id=dev(target), device_id_type=MESH), False)

    def outs_full(act, q):
        for unit in range(2, 8):
            if unit < 4:
                @pl.when(role != 2)
                def _():
                    out_copies(act, q, unit, 4 * (me - 2) + q, unit)
            else:
                out_copies(act, q, unit, 4 * (me - 2) + q, unit)

    def outs_pair(act, q):
        for unit in (2, 3, 6, 7, 0, 1, 4, 5):
            out_copies(act, q, unit, 8 + 4 * me + 2 * q + unit // 4, unit % 4)

    def outs_quad(act, q):
        for unit in range(8):
            out_copies(act, q, unit, 16 * me + 4 * (q - 2) + unit // 2, unit % 2)

    def compute():
        def sweep(q, cps, bufs):
            base = [k // cps * (pad + cps * blk) + pad + k % cps * blk for k in range(8)]

            pltpu.make_async_copy(xbuf.at[q], xbuf.at[q], x_recv.at[q]).wait()
            for k in range(8):
                bufs[0][pl.ds(base[k], blk), :] = xbuf[q, k].astype(F32)
                skip_v[q, k] = jnp.zeros((blk, chan), F32)

            def gates(l, dil, par, k):
                lhs = jnp.concatenate([bufs[par][pl.ds(base[k], blk), :], bufs[par][pl.ds(base[k] - dil, blk), :]], axis=1).astype(BF16)
                return jnp.dot(lhs, wg_v[l], preferred_element_type=F32)

            def activate(l, pre):
                act = (jnp.tanh(pre[:, :chan]) * (1.0 + jnp.tanh(pre[:, chan:]))).astype(BF16)
                return jnp.dot(act, wo_v[l], preferred_element_type=F32)

            def update(par, k, mixed):
                bufs[1 - par][pl.ds(base[k], blk), :] = bufs[par][pl.ds(base[k], blk), :] + mixed[:, :chan]
                skip_v[q, k] = skip_v[q, k] + mixed[:, chan:]

            def cycle(r, carry):
                steps = [(c, k) for c in range(n_cyc) for k in range(8)]
                pre, mixed = {}, {}
                for t in range(len(steps) + 2 * LAG):
                    if t < len(steps):
                        c, k = steps[t]
                        pre[t] = gates(r * n_cyc + c, 2**c, c % 2, k)
                    if 0 <= t - LAG < len(steps):
                        c, k = steps[t - LAG]
                        mixed[t - LAG] = activate(r * n_cyc + c, pre.pop(t - LAG))
                    if 0 <= t - 2 * LAG:
                        c, k = steps[t - 2 * LAG]
                        update(c % 2, k, mixed.pop(t - 2 * LAG))
                return carry

            lax.fori_loop(0, n_layers // n_cyc, cycle, 0)
            for k in range(8):
                hout_v[q, k] = bufs[0][pl.ds(base[k], blk), :]

        @pl.when(role == 0)
        def _():
            @pl.loop(0, 2)
            def _(q):
                sweep(q, 4, (ha1, hb1))
                outs_pair(lambda copy, local: copy.start(), q)

            @pl.loop(2, 4)
            def _(q):
                sweep(q, 2, (ha2, hb2))
                outs_quad(lambda copy, local: copy.start(), q)

        @pl.when(role != 0)
        def _():
            @pl.loop(0, 4)
            def _(q):
                sweep(q, 8, (ha0, hb0))
                outs_full(lambda copy, local: copy.start(), q)

    compute()

    def sent(copy, local):
        if not local:
            copy.wait_send()

    x_copies(sent)

    @pl.when(role == 0)
    def _():
        @pl.loop(0, 2)
        def _(q):
            outs_pair(sent, q)

        @pl.loop(2, 4)
        def _(q):
            outs_quad(sent, q)

    @pl.when(role != 0)
    def _():
        @pl.loop(0, 4)
        def _(q):
            outs_full(sent, q)

    pltpu.make_async_copy(h_out, h_out, h_recv).wait()
    pltpu.make_async_copy(s_out, s_out, s_recv).wait()


def solution(mesh):
    seq_spec = P("batch", SEQ_AXES, None)

    def local_stack(x_loc, w_f0, w_f1, w_g0, w_g1, w_res, w_skip):
        n_rep, n_cyc, chan = w_f0.shape[:3]
        n_layers = n_rep * n_cyc
        n_seq, blk, _ = x_loc.shape
        pad = 2 ** (n_cyc - 1)
        weights = [w.reshape(n_layers, chan, chan) for w in (w_f0, w_f1, w_g0, w_g1, w_res, w_skip)]
        any_spec = pl.BlockSpec(memory_space=pl.ANY)
        out = jax.ShapeDtypeStruct((n_seq, blk, chan), F32)
        return pl.pallas_call(
            functools.partial(kernel, n_layers, n_cyc, blk, pad),
            out_shape=(out, out),
            in_specs=[any_spec] * 7,
            out_specs=(any_spec, any_spec),
            scratch_shapes=[
                pltpu.VMEM((4, 8, blk, chan), BF16),
                pltpu.VMEM((n_layers, 2 * chan, 2 * chan), BF16),
                pltpu.VMEM((n_layers, chan, 2 * chan), BF16),
                pltpu.VMEM((pad + 8 * blk, chan), F32),
                pltpu.VMEM((pad + 8 * blk, chan), F32),
                pltpu.VMEM((2 * pad + 8 * blk, chan), F32),
                pltpu.VMEM((2 * pad + 8 * blk, chan), F32),
                pltpu.VMEM((4 * pad + 8 * blk, chan), F32),
                pltpu.VMEM((4 * pad + 8 * blk, chan), F32),
                pltpu.VMEM((4, 8, blk, chan), F32),
                pltpu.VMEM((4, 8, blk, chan), F32),
                pltpu.SemaphoreType.DMA((6,)),
                pltpu.SemaphoreType.DMA,
                pltpu.SemaphoreType.DMA((4,)),
                pltpu.SemaphoreType.DMA,
                pltpu.SemaphoreType.DMA,
                pltpu.SemaphoreType.DMA,
            ],
            compiler_params=pltpu.CompilerParams(collective_id=0, has_side_effects=True, vmem_limit_bytes=60 * 2**20),
        )(x_loc, *weights)

    return jax.shard_map(local_stack, mesh=mesh, in_specs=(seq_spec, P(), P(), P(), P(), P(), P()), out_specs=(seq_spec, seq_spec), check_vma=False)
```

```python
import functools

import jax
import jax.numpy as jnp
from jax import lax
from jax.experimental import pallas as pl
from jax.experimental.pallas import tpu as pltpu
from jax.sharding import PartitionSpec as P

MESH = pl.DeviceIdType.MESH
SEQ_AXES = ("seq_hi", "seq")
N_DEV = 8
PIECES = 4
LAG = 2
F32 = jnp.float32
BF16 = jnp.bfloat16


def kernel(n_layers, n_cyc, blk, pad, x_ref, wf0, wf1, wg0, wg1, wr, ws, h_out, s_out,
           xbuf, wg_v, wo_v, ha0, hb0, ha1, hb1, ha2, hb2, hout_v, skip_v,
           w_sem, x_send, x_recv, o_send, h_recv, s_recv):
    hi, lo = lax.axis_index("seq_hi"), lax.axis_index("seq")
    me = hi * 4 + lo
    role = me // 2
    chan = x_ref.shape[-1]

    def dev(index):
        return {"seq_hi": index // 4, "seq": index % 4}

    w_copies = [
        pltpu.make_async_copy(wf1, wg_v.at[:, pl.ds(0, chan), pl.ds(0, chan)], w_sem.at[0]),
        pltpu.make_async_copy(wg1, wg_v.at[:, pl.ds(0, chan), pl.ds(chan, chan)], w_sem.at[1]),
        pltpu.make_async_copy(wf0, wg_v.at[:, pl.ds(chan, chan), pl.ds(0, chan)], w_sem.at[2]),
        pltpu.make_async_copy(wg0, wg_v.at[:, pl.ds(chan, chan), pl.ds(chan, chan)], w_sem.at[3]),
        pltpu.make_async_copy(wr, wo_v.at[:, :, pl.ds(0, chan)], w_sem.at[4]),
        pltpu.make_async_copy(ws, wo_v.at[:, :, pl.ds(chan, chan)], w_sem.at[5]),
    ]
    for copy in w_copies:
        copy.start()

    barrier = pltpu.get_barrier_semaphore()
    for other in range(N_DEV):
        @pl.when(me != other)
        def _():
            pl.semaphore_signal(barrier, inc=1, device_id=dev(other), device_id_type=MESH)
    pl.semaphore_wait(barrier, N_DEV - 1)

    def x_copies(act):
        def one(seq, target, q, unit):
            @pl.when(me == target)
            def _():
                act(pltpu.make_async_copy(x_ref.at[seq], xbuf.at[q, unit], x_recv.at[q]), True)

            @pl.when(me != target)
            def _():
                act(pltpu.make_async_remote_copy(
                    src_ref=x_ref.at[seq], dst_ref=xbuf.at[q, unit], send_sem=x_send, recv_sem=x_recv.at[q],
                    device_id=dev(target), device_id_type=MESH), False)

        for q in range(4):
            for target in range(2):
                if q < 2:
                    @pl.when(me < 4)
                    def _():
                        for half in range(2):
                            one(8 + 4 * target + 2 * q + half, target, q, half * 4 + me)
                else:
                    @pl.when(me < 2)
                    def _():
                        for part in range(4):
                            one(16 * target + 4 * (q - 2) + part, target, q, part * 2 + me)
            for target in range(2, N_DEV):
                one(4 * (target - 2) + q, target, q, me)

    x_copies(lambda copy, local: copy.start())

    def zero_pads(bufs, cps):
        for buf in bufs:
            for first in range(0, 8, cps):
                buf[pl.ds(first // cps * (pad + cps * blk), pad), :] = jnp.zeros((pad, chan), F32)

    @pl.when(role == 0)
    def _():
        zero_pads((ha1, hb1), 4)
        zero_pads((ha2, hb2), 2)

    @pl.when(role != 0)
    def _():
        zero_pads((ha0, hb0), 8)

    for copy in w_copies:
        copy.wait()

    def halve(l, carry):
        wg_v[l, :, pl.ds(chan, chan)] = wg_v[l, :, pl.ds(chan, chan)] * BF16(0.5)
        wo_v[l] = wo_v[l] * BF16(0.5)
        return carry

    lax.fori_loop(0, n_layers, halve, 0)

    def out_copies(act, start, q, unit, seq, target):
        for src, dst, recv in ((hout_v, h_out, h_recv), (skip_v, s_out, s_recv)):
            @pl.when(me == target)
            def _():
                if start:
                    dst[seq] = src[q, unit]

            @pl.when(me != target)
            def _():
                act(pltpu.make_async_remote_copy(
                    src_ref=src.at[q, unit], dst_ref=dst.at[seq], send_sem=o_send, recv_sem=recv,
                    device_id=dev(target), device_id_type=MESH))

    def outs_full(act, start, q):
        for unit in range(2, 8):
            if unit < 4:
                @pl.when(role != 2)
                def _():
                    out_copies(act, start, q, unit, 4 * (me - 2) + q, unit)
            else:
                out_copies(act, start, q, unit, 4 * (me - 2) + q, unit)

    def outs_pair(act, start, q):
        for unit in (2, 3, 6, 7, 0, 1, 4, 5):
            out_copies(act, start, q, unit, 8 + 4 * me + 2 * q + unit // 4, unit % 4)

    def outs_quad(act, start, q):
        for unit in range(8):
            out_copies(act, start, q, unit, 16 * me + 4 * (q - 2) + unit // 2, unit % 2)

    def compute():
        def sweep(q, cps, bufs):
            base = [k // cps * (pad + cps * blk) + pad + k % cps * blk for k in range(8)]

            pltpu.make_async_copy(xbuf.at[q], xbuf.at[q], x_recv.at[q]).wait()
            for k in range(8):
                bufs[0][pl.ds(base[k], blk), :] = xbuf[q, k].astype(F32)
                skip_v[q, k] = jnp.zeros((blk, chan), F32)

            def gates(l, dil, par, k):
                lhs = jnp.concatenate([bufs[par][pl.ds(base[k], blk), :], bufs[par][pl.ds(base[k] - dil, blk), :]], axis=1).astype(BF16)
                return jnp.dot(lhs, wg_v[l], preferred_element_type=F32)

            def activate(l, pre):
                act = (jnp.tanh(pre[:, :chan]) * (1.0 + jnp.tanh(pre[:, chan:]))).astype(BF16)
                return jnp.dot(act, wo_v[l], preferred_element_type=F32)

            def update(par, k, mixed):
                bufs[1 - par][pl.ds(base[k], blk), :] = bufs[par][pl.ds(base[k], blk), :] + mixed[:, :chan]
                skip_v[q, k] = skip_v[q, k] + mixed[:, chan:]

            def cycle(r, carry):
                steps = [(c, k) for c in range(n_cyc) for k in range(8)]
                pre, mixed = {}, {}
                for t in range(len(steps) + 2 * LAG):
                    if t < len(steps):
                        c, k = steps[t]
                        pre[t] = gates(r * n_cyc + c, 2**c, c % 2, k)
                    if 0 <= t - LAG < len(steps):
                        c, k = steps[t - LAG]
                        mixed[t - LAG] = activate(r * n_cyc + c, pre.pop(t - LAG))
                    if 0 <= t - 2 * LAG:
                        c, k = steps[t - 2 * LAG]
                        update(c % 2, k, mixed.pop(t - 2 * LAG))
                return carry

            lax.fori_loop(0, n_layers // n_cyc, cycle, 0)
            for k in range(8):
                hout_v[q, k] = bufs[0][pl.ds(base[k], blk), :]

        @pl.when(role == 0)
        def _():
            @pl.loop(0, 2)
            def _(q):
                sweep(q, 4, (ha1, hb1))
                outs_pair(lambda copy: copy.start(), True, q)

            @pl.loop(2, 4)
            def _(q):
                sweep(q, 2, (ha2, hb2))
                outs_quad(lambda copy: copy.start(), True, q)

        @pl.when(role != 0)
        def _():
            @pl.loop(0, 4)
            def _(q):
                sweep(q, 8, (ha0, hb0))
                outs_full(lambda copy: copy.start(), True, q)

    compute()

    def sent(copy, local):
        if not local:
            copy.wait_send()

    x_copies(sent)

    @pl.when(role == 0)
    def _():
        @pl.loop(0, 2)
        def _(q):
            outs_pair(lambda copy: copy.wait_send(), False, q)

        @pl.loop(2, 4)
        def _(q):
            outs_quad(lambda copy: copy.wait_send(), False, q)

    @pl.when(role != 0)
    def _():
        @pl.loop(0, 4)
        def _(q):
            outs_full(lambda copy: copy.wait_send(), False, q)

    def arrived(count):
        for dst, recv in ((h_out, h_recv), (s_out, s_recv)):
            part = dst.at[pl.ds(0, count)]
            pltpu.make_async_copy(part, part, recv).wait()

    @pl.when(role == 0)
    def _():
        arrived(12)

    @pl.when(role != 0)
    def _():
        arrived(20)


def to_hbm(h_vmem, s_vmem, h_hbm, s_hbm, sems):
    piece = h_vmem.shape[0] // PIECES
    copies = []
    for i in range(PIECES):
        rows = pl.ds(i * piece, piece)
        for j, (src, dst) in enumerate(((h_vmem, h_hbm), (s_vmem, s_hbm))):
            copies.append(pltpu.make_async_copy(src.at[rows], dst.at[rows], sems.at[j, i]))
    for copy in copies:
        copy.start()
    for copy in copies:
        copy.wait()


def solution(mesh):
    seq_spec = P("batch", SEQ_AXES, None)

    def local_stack(x_loc, w_f0, w_f1, w_g0, w_g1, w_res, w_skip):
        n_rep, n_cyc, chan = w_f0.shape[:3]
        n_layers = n_rep * n_cyc
        n_seq, blk, _ = x_loc.shape
        pad = 2 ** (n_cyc - 1)
        weights = [w.reshape(n_layers, chan, chan) for w in (w_f0, w_f1, w_g0, w_g1, w_res, w_skip)]
        any_spec = pl.BlockSpec(memory_space=pl.ANY)
        out = jax.ShapeDtypeStruct((n_seq, blk, chan), F32)
        vmem_spec = pl.BlockSpec(memory_space=pltpu.VMEM)
        vmem_out = pltpu.VMEM((n_seq, blk, chan), F32)
        landed = pl.pallas_call(
            functools.partial(kernel, n_layers, n_cyc, blk, pad),
            out_shape=(vmem_out, vmem_out),
            in_specs=[pl.BlockSpec(memory_space=pltpu.HBM)] * 7,
            out_specs=(vmem_spec, vmem_spec),
            scratch_shapes=[
                pltpu.VMEM((4, 8, blk, chan), BF16),
                pltpu.VMEM((n_layers, 2 * chan, 2 * chan), BF16),
                pltpu.VMEM((n_layers, chan, 2 * chan), BF16),
                pltpu.VMEM((pad + 8 * blk, chan), F32),
                pltpu.VMEM((pad + 8 * blk, chan), F32),
                pltpu.VMEM((2 * pad + 8 * blk, chan), F32),
                pltpu.VMEM((2 * pad + 8 * blk, chan), F32),
                pltpu.VMEM((4 * pad + 8 * blk, chan), F32),
                pltpu.VMEM((4 * pad + 8 * blk, chan), F32),
                pltpu.VMEM((4, 8, blk, chan), F32),
                pltpu.VMEM((4, 8, blk, chan), F32),
                pltpu.SemaphoreType.DMA((6,)),
                pltpu.SemaphoreType.DMA,
                pltpu.SemaphoreType.DMA((4,)),
                pltpu.SemaphoreType.DMA,
                pltpu.SemaphoreType.DMA,
                pltpu.SemaphoreType.DMA,
            ],
            compiler_params=pltpu.CompilerParams(collective_id=0, has_side_effects=True, vmem_limit_bytes=40 * 2**20),
        )(*[pltpu.with_memory_space_constraint(v, pltpu.HBM) for v in (x_loc, *weights)])
        return pl.pallas_call(
            to_hbm,
            out_shape=(out, out),
            in_specs=[vmem_spec, vmem_spec],
            out_specs=(any_spec, any_spec),
            scratch_shapes=[pltpu.SemaphoreType.DMA((2, PIECES))],
            compiler_params=pltpu.CompilerParams(vmem_limit_bytes=2 * 2**20),
        )(*landed)

    return jax.shard_map(local_stack, mesh=mesh, in_specs=(seq_spec, P(), P(), P(), P(), P(), P()), out_specs=(seq_spec, seq_spec), check_vma=False)
```

```python
import functools

import jax
import jax.numpy as jnp
from jax import lax
from jax.experimental import pallas as pl
from jax.experimental.pallas import tpu as pltpu
from jax.sharding import PartitionSpec as P

MESH = pl.DeviceIdType.MESH
SEQ_AXES = ("seq_hi", "seq")
N_DEV = 8
PIECES = 4
LAG = 2
F32 = jnp.float32
BF16 = jnp.bfloat16

PLAN = (
    (
        ((8, 4, (0, 1, 2, 3)), (9, 4, (0, 1, 2, 3)),),
        ((10, 4, (0, 1, 2, 3)), (11, 4, (0, 1, 2, 3)),),
        ((0, 2, (0, 1)), (1, 2, (0, 1)), (2, 2, (0, 1)), (3, 2, (0, 1)),),
        ((4, 2, (0, 1)), (5, 2, (0, 1)), (6, 2, (0, 1)), (7, 2, (0, 1)),),
    ),
    (
        ((12, 4, (0, 1, 2, 3)), (13, 4, (0, 1, 2, 3)),),
        ((14, 4, (0, 1, 2, 3)), (15, 4, (0, 1, 2, 3)),),
        ((16, 2, (0, 1)), (17, 2, (0, 1)), (18, 2, (0, 1)), (19, 2, (0, 1)),),
        ((20, 2, (0, 1)), (21, 2, (0, 1)), (22, 2, (0, 1)), (23, 2, (0, 1)),),
    ),
    (
        ((0, 8, (2, 3, 4, 5, 6, 7)),),
        ((1, 8, (2, 3, 4, 5, 6, 7)),),
        ((2, 8, (2, 3, 4, 5, 6, 7)),),
        ((3, 8, (2, 3, 4, 5, 6, 7)),),
    ),
    (
        ((4, 8, (2, 3, 4, 5, 6, 7)),),
        ((5, 8, (2, 3, 4, 5, 6, 7)),),
        ((6, 8, (2, 3, 4, 5, 6, 7)),),
        ((7, 8, (2, 3, 4, 5, 6, 7)),),
    ),
    (
        ((8, 8, (4, 5, 6, 7)),),
        ((9, 8, (4, 5, 6, 7)),),
        ((10, 8, (4, 5, 6, 7)),),
        ((11, 8, (4, 5, 6, 7)),),
    ),
    (
        ((12, 8, (4, 5, 6, 7)),),
        ((13, 8, (4, 5, 6, 7)),),
        ((14, 8, (4, 5, 6, 7)),),
        ((15, 8, (4, 5, 6, 7)),),
    ),
    (
        ((16, 8, (2, 3, 4, 5, 6, 7)),),
        ((17, 8, (2, 3, 4, 5, 6, 7)),),
        ((18, 8, (2, 3, 4, 5, 6, 7)),),
        ((19, 8, (2, 3, 4, 5, 6, 7)),),
    ),
    (
        ((20, 8, (2, 3, 4, 5, 6, 7)),),
        ((21, 8, (2, 3, 4, 5, 6, 7)),),
        ((22, 8, (2, 3, 4, 5, 6, 7)),),
        ((23, 8, (2, 3, 4, 5, 6, 7)),),
    ),
)
N_SWEEP = max(len(sweeps) for sweeps in PLAN)
KINDS = tuple(sorted({tuple(n for _, n, _ in sweep) for sweeps in PLAN for sweep in sweeps}, reverse=True))


def units(sweep):
    return [(k, *rest) for k, rest in enumerate((seq, b, b in keep) for seq, n, keep in sweep for b in range(n))]


def kernel(n_layers, n_cyc, blk, pad, x_ref, wf0, wf1, wg0, wg1, wr, ws, h_out, s_out,
           x_own, xbuf, wg_v, wo_v, hout_v, skip_v, w_sem, own_sem, x_send, x_recv, o_send, h_recv, s_recv, *state):
    me = lax.axis_index("seq_hi") * 4 + lax.axis_index("seq")
    chan = x_ref.shape[-1]
    n_seq = x_ref.shape[0]
    bufs_of = {kind: state[2 * i:2 * i + 2] for i, kind in enumerate(KINDS)}

    def dev(index):
        return {"seq_hi": index // 4, "seq": index % 4}

    def on(index):
        return pl.when(me == index)

    own = pltpu.make_async_copy(x_ref, x_own, own_sem)
    own.start()
    w_copies = [
        pltpu.make_async_copy(wf1, wg_v.at[:, pl.ds(0, chan), pl.ds(0, chan)], w_sem.at[0]),
        pltpu.make_async_copy(wg1, wg_v.at[:, pl.ds(0, chan), pl.ds(chan, chan)], w_sem.at[1]),
        pltpu.make_async_copy(wf0, wg_v.at[:, pl.ds(chan, chan), pl.ds(0, chan)], w_sem.at[2]),
        pltpu.make_async_copy(wg0, wg_v.at[:, pl.ds(chan, chan), pl.ds(chan, chan)], w_sem.at[3]),
        pltpu.make_async_copy(wr, wo_v.at[:, :, pl.ds(0, chan)], w_sem.at[4]),
        pltpu.make_async_copy(ws, wo_v.at[:, :, pl.ds(chan, chan)], w_sem.at[5]),
    ]
    for copy in w_copies:
        copy.start()

    barrier = pltpu.get_barrier_semaphore()
    for step in range(1, N_DEV):
        other = lax.rem(me + step, N_DEV)
        pl.semaphore_signal(barrier, inc=1, device_id={"seq_hi": other // 4, "seq": lax.rem(other, 4)}, device_id_type=MESH)
    pl.semaphore_wait(barrier, N_DEV - 1)
    own.wait()

    wanted = [[] for _ in range(N_DEV)]
    for target, sweeps in enumerate(PLAN):
        for q, sweep in enumerate(sweeps):
            for k, seq, b, _ in units(sweep):
                wanted[b].append((q, (target // 2) ^ (b // 2) != 3, target, k, seq))
    for src in range(N_DEV):
        @on(src)
        def _():
            for q, _, target, k, seq in sorted(wanted[src]):
                if target == src:
                    pltpu.make_async_copy(x_ref.at[seq], xbuf.at[q, k], x_recv.at[q]).start()
                else:
                    pltpu.make_async_remote_copy(
                        src_ref=x_own.at[seq], dst_ref=xbuf.at[q, k], send_sem=x_send, recv_sem=x_recv.at[q],
                        device_id=dev(target), device_id_type=MESH).start()

    for kind in KINDS:
        users = [d for d in range(N_DEV) if any(tuple(n for _, n, _ in sweep) == kind for sweep in PLAN[d])]
        uses = functools.reduce(jnp.logical_or, [me == d for d in users])

        @pl.when(uses)
        def _():
            first = 0
            for n in kind:
                for buf in bufs_of[kind]:
                    buf[pl.ds(first, pad), :] = jnp.zeros((pad, chan), F32)
                first += pad + n * blk

    for copy in w_copies:
        copy.wait()

    def halve(l, carry):
        wg_v[l, :, pl.ds(chan, chan)] = wg_v[l, :, pl.ds(chan, chan)] * BF16(0.5)
        wo_v[l] = wo_v[l] * BF16(0.5)
        return carry

    lax.fori_loop(0, n_layers, halve, 0)

    def compute(q, kind):
        bufs = bufs_of[kind]
        base, first = [], 0
        for n in kind:
            base += [first + pad + b * blk for b in range(n)]
            first += pad + n * blk
        count = len(base)
        lag = LAG if count > 4 else 1

        arrived = xbuf.at[q, pl.ds(0, count)]
        pltpu.make_async_copy(arrived, arrived, x_recv.at[q]).wait()
        for k in range(count):
            bufs[0][pl.ds(base[k], blk), :] = xbuf[q, k].astype(F32)
            skip_v[q, k] = jnp.zeros((blk, chan), F32)

        def gates(l, dil, par, k):
            lhs = jnp.concatenate([bufs[par][pl.ds(base[k], blk), :], bufs[par][pl.ds(base[k] - dil, blk), :]], axis=1).astype(BF16)
            return jnp.dot(lhs, wg_v[l], preferred_element_type=F32)

        def activate(l, pre):
            act = (jnp.tanh(pre[:, :chan]) * (1.0 + jnp.tanh(pre[:, chan:]))).astype(BF16)
            return jnp.dot(act, wo_v[l], preferred_element_type=F32)

        def update(par, k, mixed):
            bufs[1 - par][pl.ds(base[k], blk), :] = bufs[par][pl.ds(base[k], blk), :] + mixed[:, :chan]
            skip_v[q, k] = skip_v[q, k] + mixed[:, chan:]

        def cycle(r, carry):
            steps = [(c, k) for c in range(n_cyc) for k in range(count)]
            pre, mixed = {}, {}
            for t in range(len(steps) + 2 * lag):
                if t < len(steps):
                    c, k = steps[t]
                    pre[t] = gates(r * n_cyc + c, 2**c, c % 2, k)
                if 0 <= t - lag < len(steps):
                    c, k = steps[t - lag]
                    mixed[t - lag] = activate(r * n_cyc + c, pre.pop(t - lag))
                if 0 <= t - 2 * lag:
                    c, k = steps[t - 2 * lag]
                    update(c % 2, k, mixed.pop(t - 2 * lag))
            return carry

        lax.fori_loop(0, n_layers // n_cyc, cycle, 0)
        for k in range(count):
            hout_v[q, k] = bufs[0][pl.ds(base[k], blk), :]

    def deliver(src, q):
        out = [(k, seq, b) for k, seq, b, counts in units(PLAN[src][q]) if counts]
        for k, seq, b in sorted(out, key=lambda u: ((src // 2) ^ (u[2] // 2) != 3, u)):
            for part, dst, recv in ((hout_v, h_out, h_recv), (skip_v, s_out, s_recv)):
                if b == src:
                    dst[seq] = part[q, k]
                else:
                    pltpu.make_async_remote_copy(
                        src_ref=part.at[q, k], dst_ref=dst.at[seq], send_sem=o_send, recv_sem=recv,
                        device_id=dev(b), device_id_type=MESH).start()

    def run(q, carry):
        for kind in KINDS:
            where = [(d, i) for d in range(N_DEV) for i, sweep in enumerate(PLAN[d]) if tuple(n for _, n, _ in sweep) == kind]
            hit = functools.reduce(jnp.logical_or, [jnp.logical_and(me == d, q == i) for d, i in where])

            @pl.when(hit)
            def _():
                compute(q, kind)

        for d in range(N_DEV):
            @on(d)
            def _():
                for i in range(len(PLAN[d])):
                    @pl.when(q == i)
                    def _():
                        deliver(d, i)
        return carry

    lax.fori_loop(0, N_SWEEP, run, 0)

    def drain(ref, sem, count):
        while count > 0:
            part = ref.at[pl.ds(0, min(count, n_seq))]
            pltpu.make_async_copy(part, part, sem).wait()
            count -= n_seq

    for d in range(N_DEV):
        @on(d)
        def _():
            drain(x_own, x_send, sum(target != d for _, _, target, _, _ in wanted[d]))
            results = [b for q in range(len(PLAN[d])) for _, _, b, counts in units(PLAN[d][q]) if counts]
            kept = results.count(d)
            drain(h_out, o_send, 2 * (len(results) - kept))
            drain(h_out, h_recv, n_seq - kept)
            drain(s_out, s_recv, n_seq - kept)


def to_hbm(h_vmem, s_vmem, h_hbm, s_hbm, sems):
    piece = h_vmem.shape[0] // PIECES
    copies = []
    for i in range(PIECES):
        rows = pl.ds(i * piece, piece)
        for j, (src, dst) in enumerate(((h_vmem, h_hbm), (s_vmem, s_hbm))):
            copies.append(pltpu.make_async_copy(src.at[rows], dst.at[rows], sems.at[j, i]))
    for copy in copies:
        copy.start()
    for copy in copies:
        copy.wait()


def solution(mesh):
    seq_spec = P("batch", SEQ_AXES, None)

    def local_stack(x_loc, w_f0, w_f1, w_g0, w_g1, w_res, w_skip):
        n_rep, n_cyc, chan = w_f0.shape[:3]
        n_layers = n_rep * n_cyc
        n_seq, blk, _ = x_loc.shape
        pad = 2 ** (n_cyc - 1)
        weights = [w.reshape(n_layers, chan, chan) for w in (w_f0, w_f1, w_g0, w_g1, w_res, w_skip)]
        any_spec = pl.BlockSpec(memory_space=pl.ANY)
        vmem_spec = pl.BlockSpec(memory_space=pltpu.VMEM)
        out = jax.ShapeDtypeStruct((n_seq, blk, chan), F32)
        vmem_out = pltpu.VMEM((n_seq, blk, chan), F32)
        state = [pltpu.VMEM((sum(pad + n * blk for n in kind), chan), F32) for kind in KINDS for _ in range(2)]
        landed = pl.pallas_call(
            functools.partial(kernel, n_layers, n_cyc, blk, pad),
            out_shape=(vmem_out, vmem_out),
            in_specs=[any_spec] * 7,
            out_specs=(vmem_spec, vmem_spec),
            scratch_shapes=[
                pltpu.VMEM((n_seq, blk, chan), BF16),
                pltpu.VMEM((N_SWEEP, 8, blk, chan), BF16),
                pltpu.VMEM((n_layers, 2 * chan, 2 * chan), BF16),
                pltpu.VMEM((n_layers, chan, 2 * chan), BF16),
                pltpu.VMEM((N_SWEEP, 8, blk, chan), F32),
                pltpu.VMEM((N_SWEEP, 8, blk, chan), F32),
                pltpu.SemaphoreType.DMA((6,)),
                pltpu.SemaphoreType.DMA,
                pltpu.SemaphoreType.DMA,
                pltpu.SemaphoreType.DMA((N_SWEEP,)),
                pltpu.SemaphoreType.DMA,
                pltpu.SemaphoreType.DMA,
                pltpu.SemaphoreType.DMA,
                *state,
            ],
            compiler_params=pltpu.CompilerParams(collective_id=0, has_side_effects=True, vmem_limit_bytes=44 * 2**20),
        )(*[pltpu.with_memory_space_constraint(v, pltpu.HBM) for v in (x_loc, *weights)])
        return pl.pallas_call(
            to_hbm,
            out_shape=(out, out),
            in_specs=[vmem_spec, vmem_spec],
            out_specs=(any_spec, any_spec),
            scratch_shapes=[pltpu.SemaphoreType.DMA((2, PIECES))],
            compiler_params=pltpu.CompilerParams(vmem_limit_bytes=2 * 2**20),
        )(*landed)

    return jax.shard_map(local_stack, mesh=mesh, in_specs=(seq_spec, P(), P(), P(), P(), P(), P()), out_specs=(seq_spec, seq_spec), check_vma=False)
```

```python
import functools

import jax
import jax.numpy as jnp
from jax import lax
from jax.experimental import pallas as pl
from jax.experimental.pallas import tpu as pltpu
from jax.sharding import PartitionSpec as P

MESH = pl.DeviceIdType.MESH
SEQ_AXES = ("seq_hi", "seq")
N_DEV = 8
PIECES = 4
LAG = 2
F32 = jnp.float32
BF16 = jnp.bfloat16

PLAN = (
    (
        ((8, 4, (0, 1, 2, 3)), (9, 4, (0, 1, 2, 3)),),
        ((10, 4, (0, 1, 2, 3)), (11, 4, (0, 1, 2, 3)),),
        ((0, 2, (0, 1)), (1, 2, (0, 1)), (2, 2, (0, 1)), (3, 2, (0, 1)),),
        ((4, 2, (0, 1)), (5, 2, (0, 1)), (6, 2, (0, 1)), (7, 2, (0, 1)),),
    ),
    (
        ((12, 4, (0, 1, 2, 3)), (13, 4, (0, 1, 2, 3)),),
        ((14, 4, (0, 1, 2, 3)), (15, 4, (0, 1, 2, 3)),),
        ((16, 2, (0, 1)), (17, 2, (0, 1)), (18, 2, (0, 1)), (19, 2, (0, 1)),),
        ((20, 2, (0, 1)), (21, 2, (0, 1)), (22, 2, (0, 1)), (23, 2, (0, 1)),),
    ),
    (
        ((0, 8, (2, 3, 4, 5, 6, 7)),),
        ((1, 8, (2, 3, 4, 5, 6, 7)),),
        ((2, 8, (2, 3, 4, 5, 6, 7)),),
        ((3, 8, (2, 3, 4, 5, 6, 7)),),
    ),
    (
        ((4, 8, (2, 3, 4, 5, 6, 7)),),
        ((5, 8, (2, 3, 4, 5, 6, 7)),),
        ((6, 8, (2, 3, 4, 5, 6, 7)),),
        ((7, 8, (2, 3, 4, 5, 6, 7)),),
    ),
    (
        ((8, 8, (4, 5, 6, 7)),),
        ((9, 8, (4, 5, 6, 7)),),
        ((10, 8, (4, 5, 6, 7)),),
        ((11, 8, (4, 5, 6, 7)),),
    ),
    (
        ((12, 8, (4, 5, 6, 7)),),
        ((13, 8, (4, 5, 6, 7)),),
        ((14, 8, (4, 5, 6, 7)),),
        ((15, 8, (4, 5, 6, 7)),),
    ),
    (
        ((16, 8, (2, 3, 4, 5, 6, 7)),),
        ((17, 8, (2, 3, 4, 5, 6, 7)),),
        ((18, 8, (2, 3, 4, 5, 6, 7)),),
        ((19, 8, (2, 3, 4, 5, 6, 7)),),
    ),
    (
        ((20, 8, (2, 3, 4, 5, 6, 7)),),
        ((21, 8, (2, 3, 4, 5, 6, 7)),),
        ((22, 8, (2, 3, 4, 5, 6, 7)),),
        ((23, 8, (2, 3, 4, 5, 6, 7)),),
    ),
)
N_SWEEP = max(len(sweeps) for sweeps in PLAN)
KINDS = tuple(sorted({tuple(n for _, n, _ in sweep) for sweeps in PLAN for sweep in sweeps}, reverse=True))


def units(sweep):
    return [(k, *rest) for k, rest in enumerate((seq, b, b in keep) for seq, n, keep in sweep for b in range(n))]


def kernel(n_layers, n_cyc, blk, pad, x_ref, wf0, wf1, wg0, wg1, wr, ws, h_out, s_out,
           x_own, xbuf, wg_v, wo_v, hout_v, skip_v, w_sem, own_sem, x_send, x_recv, o_send, h_recv, s_recv, *state):
    me = lax.axis_index("seq_hi") * 4 + lax.axis_index("seq")
    chan = x_ref.shape[-1]
    n_seq = x_ref.shape[0]
    bufs_of = {kind: state[2 * i:2 * i + 2] for i, kind in enumerate(KINDS)}

    def dev(index):
        return {"seq_hi": index // 4, "seq": index % 4}

    def on(index):
        return pl.when(me == index)

    own = pltpu.make_async_copy(x_ref, x_own, own_sem)
    own.start()
    w_copies = [
        pltpu.make_async_copy(wf1, wg_v.at[:, pl.ds(0, chan), pl.ds(0, chan)], w_sem.at[0]),
        pltpu.make_async_copy(wg1, wg_v.at[:, pl.ds(0, chan), pl.ds(chan, chan)], w_sem.at[1]),
        pltpu.make_async_copy(wf0, wg_v.at[:, pl.ds(chan, chan), pl.ds(0, chan)], w_sem.at[2]),
        pltpu.make_async_copy(wg0, wg_v.at[:, pl.ds(chan, chan), pl.ds(chan, chan)], w_sem.at[3]),
        pltpu.make_async_copy(wr, wo_v.at[:, :, pl.ds(0, chan)], w_sem.at[4]),
        pltpu.make_async_copy(ws, wo_v.at[:, :, pl.ds(chan, chan)], w_sem.at[5]),
    ]
    for copy in w_copies:
        copy.start()

    barrier = pltpu.get_barrier_semaphore()
    for step in range(1, N_DEV):
        other = lax.rem(me + step, N_DEV)
        pl.semaphore_signal(barrier, inc=1, device_id={"seq_hi": other // 4, "seq": lax.rem(other, 4)}, device_id_type=MESH)
    pl.semaphore_wait(barrier, N_DEV - 1)
    own.wait()

    wanted = [[] for _ in range(N_DEV)]
    for target, sweeps in enumerate(PLAN):
        for q, sweep in enumerate(sweeps):
            for k, seq, b, _ in units(sweep):
                wanted[b].append((q, (target // 2) ^ (b // 2) != 3, target, k, seq))
    for src in range(N_DEV):
        @on(src)
        def _():
            for q, _, target, k, seq in sorted(wanted[src]):
                if target == src:
                    pltpu.make_async_copy(x_ref.at[seq], xbuf.at[q, k], x_recv.at[q]).start()
                else:
                    pltpu.make_async_remote_copy(
                        src_ref=x_own.at[seq], dst_ref=xbuf.at[q, k], send_sem=x_send, recv_sem=x_recv.at[q],
                        device_id=dev(target), device_id_type=MESH).start()

    for kind in KINDS:
        users = [d for d in range(N_DEV) if any(tuple(n for _, n, _ in sweep) == kind for sweep in PLAN[d])]
        uses = functools.reduce(jnp.logical_or, [me == d for d in users])

        @pl.when(uses)
        def _():
            first = 0
            for n in kind:
                for buf in bufs_of[kind]:
                    buf[pl.ds(first, pad), :] = jnp.zeros((pad, chan), F32)
                first += pad + n * blk

    for copy in w_copies:
        copy.wait()

    def halve(l, carry):
        wg_v[l, :, pl.ds(chan, chan)] = wg_v[l, :, pl.ds(chan, chan)] * BF16(0.5)
        wo_v[l] = wo_v[l] * BF16(0.5)
        return carry

    lax.fori_loop(0, n_layers, halve, 0)

    def compute(q, kind):
        bufs = bufs_of[kind]
        base, first = [], 0
        for n in kind:
            base += [first + pad + b * blk for b in range(n)]
            first += pad + n * blk
        count = len(base)
        everywhere = [units(sweep) for sweeps in PLAN for sweep in sweeps if tuple(n for _, n, _ in sweep) == kind]
        unused = [k for k in range(count) if not any(listed[k][3] for listed in everywhere)]
        lag = LAG if count > 4 else 1

        arrived = xbuf.at[q, pl.ds(0, count)]
        pltpu.make_async_copy(arrived, arrived, x_recv.at[q]).wait()

        def begin(k):
            bufs[0][pl.ds(base[k], blk), :] = xbuf[q, k].astype(F32)

        def gates(l, k):
            here, dil = bufs[l % 2], 2 ** (l % n_cyc)
            lhs = jnp.concatenate([here[pl.ds(base[k], blk), :], here[pl.ds(base[k] - dil, blk), :]], axis=1).astype(BF16)
            return jnp.dot(lhs, wg_v[l], preferred_element_type=F32)

        def activate(l, pre):
            act = (jnp.tanh(pre[:, :chan]) * (1.0 + jnp.tanh(pre[:, chan:]))).astype(BF16)
            return jnp.dot(act, wo_v[l], preferred_element_type=F32)

        def update(l, k, mixed):
            new = bufs[l % 2][pl.ds(base[k], blk), :] + mixed[:, :chan]
            if l == n_layers - 1:
                hout_v[q, k] = new
            else:
                bufs[1 - l % 2][pl.ds(base[k], blk), :] = new
            skip_v[q, k] = mixed[:, chan:] if l == 0 else skip_v[q, k] + mixed[:, chan:]

        steps = [(l, k) for l in range(n_layers) for k in range(count) if l < n_layers - 1 or k not in unused]
        pre, mixed = {}, {}
        for t in range(len(steps) + 2 * lag):
            if t < len(steps):
                if t == 0:
                    begin(0)
                if t + 1 < count:
                    begin(t + 1)
                pre[t] = gates(*steps[t])
            if 0 <= t - lag < len(steps):
                mixed[t - lag] = activate(steps[t - lag][0], pre.pop(t - lag))
            if 0 <= t - 2 * lag:
                update(*steps[t - 2 * lag], mixed.pop(t - 2 * lag))

    def deliver(src, q):
        out = [(k, seq, b) for k, seq, b, counts in units(PLAN[src][q]) if counts]
        for k, seq, b in sorted(out, key=lambda u: ((src // 2) ^ (u[2] // 2) != 3, u)):
            for part, dst, recv in ((hout_v, h_out, h_recv), (skip_v, s_out, s_recv)):
                if b == src:
                    dst[seq] = part[q, k]
                else:
                    pltpu.make_async_remote_copy(
                        src_ref=part.at[q, k], dst_ref=dst.at[seq], send_sem=o_send, recv_sem=recv,
                        device_id=dev(b), device_id_type=MESH).start()

    def run(q, carry):
        for kind in KINDS:
            where = [(d, i) for d in range(N_DEV) for i, sweep in enumerate(PLAN[d]) if tuple(n for _, n, _ in sweep) == kind]
            hit = functools.reduce(jnp.logical_or, [jnp.logical_and(me == d, q == i) for d, i in where])

            @pl.when(hit)
            def _():
                compute(q, kind)

        for d in range(N_DEV):
            @on(d)
            def _():
                for i in range(len(PLAN[d])):
                    @pl.when(q == i)
                    def _():
                        deliver(d, i)
        return carry

    lax.fori_loop(0, N_SWEEP, run, 0)

    def drain(ref, sem, count):
        while count > 0:
            part = ref.at[pl.ds(0, min(count, n_seq))]
            pltpu.make_async_copy(part, part, sem).wait()
            count -= n_seq

    for d in range(N_DEV):
        @on(d)
        def _():
            drain(x_own, x_send, sum(target != d for _, _, target, _, _ in wanted[d]))
            results = [b for q in range(len(PLAN[d])) for _, _, b, counts in units(PLAN[d][q]) if counts]
            kept = results.count(d)
            drain(h_out, o_send, 2 * (len(results) - kept))
            drain(h_out, h_recv, n_seq - kept)
            drain(s_out, s_recv, n_seq - kept)


def to_hbm(h_vmem, s_vmem, h_hbm, s_hbm, sems):
    piece = h_vmem.shape[0] // PIECES
    copies = []
    for i in range(PIECES):
        rows = pl.ds(i * piece, piece)
        for j, (src, dst) in enumerate(((h_vmem, h_hbm), (s_vmem, s_hbm))):
            copies.append(pltpu.make_async_copy(src.at[rows], dst.at[rows], sems.at[j, i]))
    for copy in copies:
        copy.start()
    for copy in copies:
        copy.wait()


def solution(mesh):
    seq_spec = P("batch", SEQ_AXES, None)

    def local_stack(x_loc, w_f0, w_f1, w_g0, w_g1, w_res, w_skip):
        n_rep, n_cyc, chan = w_f0.shape[:3]
        n_layers = n_rep * n_cyc
        n_seq, blk, _ = x_loc.shape
        pad = 2 ** (n_cyc - 1)
        weights = [w.reshape(n_layers, chan, chan) for w in (w_f0, w_f1, w_g0, w_g1, w_res, w_skip)]
        any_spec = pl.BlockSpec(memory_space=pl.ANY)
        vmem_spec = pl.BlockSpec(memory_space=pltpu.VMEM)
        out = jax.ShapeDtypeStruct((n_seq, blk, chan), F32)
        vmem_out = pltpu.VMEM((n_seq, blk, chan), F32)
        state = [pltpu.VMEM((sum(pad + n * blk for n in kind), chan), F32) for kind in KINDS for _ in range(2)]
        landed = pl.pallas_call(
            functools.partial(kernel, n_layers, n_cyc, blk, pad),
            out_shape=(vmem_out, vmem_out),
            in_specs=[any_spec] * 7,
            out_specs=(vmem_spec, vmem_spec),
            scratch_shapes=[
                pltpu.VMEM((n_seq, blk, chan), BF16),
                pltpu.VMEM((N_SWEEP, 8, blk, chan), BF16),
                pltpu.VMEM((n_layers, 2 * chan, 2 * chan), BF16),
                pltpu.VMEM((n_layers, chan, 2 * chan), BF16),
                pltpu.VMEM((N_SWEEP, 8, blk, chan), F32),
                pltpu.VMEM((N_SWEEP, 8, blk, chan), F32),
                pltpu.SemaphoreType.DMA((6,)),
                pltpu.SemaphoreType.DMA,
                pltpu.SemaphoreType.DMA,
                pltpu.SemaphoreType.DMA((N_SWEEP,)),
                pltpu.SemaphoreType.DMA,
                pltpu.SemaphoreType.DMA,
                pltpu.SemaphoreType.DMA,
                *state,
            ],
            compiler_params=pltpu.CompilerParams(collective_id=0, has_side_effects=True, vmem_limit_bytes=44 * 2**20),
        )(*[pltpu.with_memory_space_constraint(v, pltpu.HBM) for v in (x_loc, *weights)])
        return pl.pallas_call(
            to_hbm,
            out_shape=(out, out),
            in_specs=[vmem_spec, vmem_spec],
            out_specs=(any_spec, any_spec),
            scratch_shapes=[pltpu.SemaphoreType.DMA((2, PIECES))],
            compiler_params=pltpu.CompilerParams(vmem_limit_bytes=2 * 2**20),
        )(*landed)

    return jax.shard_map(local_stack, mesh=mesh, in_specs=(seq_spec, P(), P(), P(), P(), P(), P()), out_specs=(seq_spec, seq_spec), check_vma=False)
```

```python
import functools

import jax
import jax.numpy as jnp
from jax import lax
from jax.experimental import pallas as pl
from jax.experimental.pallas import tpu as pltpu
from jax.sharding import PartitionSpec as P

MESH = pl.DeviceIdType.MESH
SEQ_AXES = ("seq_hi", "seq")
N_DEV = 8
PIECES = 4
LAG = 2
UNROLLED = ((8,), (4, 4))
F32 = jnp.float32
BF16 = jnp.bfloat16

PLAN = (
    (
        ((19, 2, (0, 1)), (4, 2, (0, 1)), (6, 2, (0, 1)), (21, 2, (0, 1)),),
        ((14, 6, (0, 1, 2, 3, 4, 5)),),
        ((23, 6, (0, 1, 4, 5)),),
        ((22, 4, (0, 1, 2, 3)), (16, 4, (0, 1, 2, 3)),),
        ((12, 2, (0, 1)), (3, 2, (0, 1)), (13, 2, (0, 1)), (11, 2, (0, 1)),),
    ),
    (
        ((15, 8, (0, 1, 4, 5, 6, 7)),),
        ((18, 8, (0, 1, 4, 5, 6, 7)),),
        ((20, 2, (0, 1)), (1, 2, (0, 1)), (8, 2, (0, 1)), (7, 2, (0, 1)),),
        ((10, 2, (0, 1)), (2, 2, (0, 1)), (0, 2, (0, 1)), (9, 2, (0, 1)),),
    ),
    (
        ((20, 4, (2, 3)), (10, 4, (2, 3)),),
        ((21, 8, (2, 3, 6, 7)),),
        ((23, 8, (2, 3, 6, 7)),),
        ((18, 4, (2, 3)), (9, 4, (2, 3)),),
    ),
    (
        ((13, 8, (2, 3, 4, 5, 6, 7)),),
        ((12, 8, (2, 3, 6, 7)),),
        ((5, 8, (0, 1, 2, 3, 4, 5, 6, 7)),),
        ((0, 4, (2, 3)), (17, 4, (2, 3)),),
        ((15, 4, (2, 3)), (3, 4, (2, 3)),),
    ),
    (
        ((22, 8, (4, 5, 6, 7)),),
        ((20, 8, (4, 5, 6, 7)),),
        ((3, 8, (4, 5, 6, 7)),),
        ((16, 8, (4, 5, 6, 7)),),
        ((12, 6, (4, 5)),),
    ),
    (
        ((10, 8, (4, 5, 6, 7)),),
        ((9, 8, (4, 5, 6, 7)),),
        ((17, 8, (0, 1, 4, 5, 6, 7)),),
        ((0, 8, (4, 5, 6, 7)),),
        ((21, 6, (4, 5)),),
    ),
    (
        ((8, 8, (2, 3, 4, 5, 6, 7)),),
        ((7, 8, (2, 3, 4, 5, 6, 7)),),
        ((2, 8, (2, 3, 4, 5, 6, 7)),),
        ((6, 8, (2, 3, 4, 5, 6, 7)),),
    ),
    (
        ((11, 8, (2, 3, 4, 5, 6, 7)),),
        ((4, 8, (2, 3, 4, 5, 6, 7)),),
        ((1, 8, (2, 3, 4, 5, 6, 7)),),
        ((19, 8, (2, 3, 4, 5, 6, 7)),),
        ((14, 8, (6, 7)),),
    ),
)
N_SWEEP = max(len(sweeps) for sweeps in PLAN)
KINDS = tuple(sorted({tuple(n for _, n, _ in sweep) for sweeps in PLAN for sweep in sweeps}, reverse=True))


def units(sweep):
    return [(k, *rest) for k, rest in enumerate((seq, b, b in keep) for seq, n, keep in sweep for b in range(n))]


def kernel(n_layers, n_cyc, blk, pad, x_ref, wf0, wf1, wg0, wg1, wr, ws, h_out, s_out,
           x_own, xbuf, wg_v, wo_v, hout_v, skip_v, w_sem, own_sem, x_send, x_recv, o_send, h_recv, s_recv, *state):
    me = lax.axis_index("seq_hi") * 4 + lax.axis_index("seq")
    chan = x_ref.shape[-1]
    n_seq = x_ref.shape[0]
    bufs_of = {kind: state[2 * i:2 * i + 2] for i, kind in enumerate(KINDS)}

    def dev(index):
        return {"seq_hi": index // 4, "seq": index % 4}

    def on(index):
        return pl.when(me == index)

    own = pltpu.make_async_copy(x_ref, x_own, own_sem)
    own.start()
    w_copies = [
        pltpu.make_async_copy(wf1, wg_v.at[:, pl.ds(0, chan), pl.ds(0, chan)], w_sem.at[0]),
        pltpu.make_async_copy(wg1, wg_v.at[:, pl.ds(0, chan), pl.ds(chan, chan)], w_sem.at[1]),
        pltpu.make_async_copy(wf0, wg_v.at[:, pl.ds(chan, chan), pl.ds(0, chan)], w_sem.at[2]),
        pltpu.make_async_copy(wg0, wg_v.at[:, pl.ds(chan, chan), pl.ds(chan, chan)], w_sem.at[3]),
        pltpu.make_async_copy(wr, wo_v.at[:, :, pl.ds(0, chan)], w_sem.at[4]),
        pltpu.make_async_copy(ws, wo_v.at[:, :, pl.ds(chan, chan)], w_sem.at[5]),
    ]
    for copy in w_copies:
        copy.start()

    barrier = pltpu.get_barrier_semaphore()
    for step in range(1, N_DEV):
        other = lax.rem(me + step, N_DEV)
        pl.semaphore_signal(barrier, inc=1, device_id={"seq_hi": other // 4, "seq": lax.rem(other, 4)}, device_id_type=MESH)
    pl.semaphore_wait(barrier, N_DEV - 1)
    own.wait()

    wanted = [[] for _ in range(N_DEV)]
    for target, sweeps in enumerate(PLAN):
        for q, sweep in enumerate(sweeps):
            for k, seq, b, _ in units(sweep):
                wanted[b].append((q, ((target // 2) ^ (b // 2) != 3, target % 2 == 0), target, k, seq))
    for src in range(N_DEV):
        @on(src)
        def _():
            for q, _, target, k, seq in sorted(wanted[src]):
                if target == src:
                    pltpu.make_async_copy(x_ref.at[seq], xbuf.at[q, k], x_recv.at[q]).start()
                else:
                    pltpu.make_async_remote_copy(
                        src_ref=x_own.at[seq], dst_ref=xbuf.at[q, k], send_sem=x_send, recv_sem=x_recv.at[q],
                        device_id=dev(target), device_id_type=MESH).start()

    for kind in KINDS:
        users = [d for d in range(N_DEV) if any(tuple(n for _, n, _ in sweep) == kind for sweep in PLAN[d])]
        uses = functools.reduce(jnp.logical_or, [me == d for d in users])

        @pl.when(uses)
        def _():
            first = 0
            for n in kind:
                for buf in bufs_of[kind]:
                    buf[pl.ds(first, pad), :] = jnp.zeros((pad, chan), F32)
                first += pad + n * blk

    for copy in w_copies:
        copy.wait()

    def halve(l, carry):
        wg_v[l, :, pl.ds(chan, chan)] = wg_v[l, :, pl.ds(chan, chan)] * BF16(0.5)
        wo_v[l] = wo_v[l] * BF16(0.5)
        return carry

    lax.fori_loop(0, n_layers, halve, 0)

    def compute(q, kind):
        bufs = bufs_of[kind]
        base, first = [], 0
        for n in kind:
            base += [first + pad + b * blk for b in range(n)]
            first += pad + n * blk
        count = len(base)
        everywhere = [units(sweep) for sweeps in PLAN for sweep in sweeps if tuple(n for _, n, _ in sweep) == kind]
        unused = [k for k in range(count) if not any(listed[k][3] for listed in everywhere)]
        lag = LAG if count > 4 else 1

        arrived = xbuf.at[q, pl.ds(0, count)]
        pltpu.make_async_copy(arrived, arrived, x_recv.at[q]).wait()

        def begin(k):
            bufs[0][pl.ds(base[k], blk), :] = xbuf[q, k].astype(F32)

        def gates(l, c, k):
            here = bufs[c % 2]
            lhs = jnp.concatenate([here[pl.ds(base[k], blk), :], here[pl.ds(base[k] - 2**c, blk), :]], axis=1).astype(BF16)
            return jnp.dot(lhs, wg_v[l], preferred_element_type=F32)

        def activate(l, pre):
            act = (jnp.tanh(pre[:, :chan]) * (1.0 + jnp.tanh(pre[:, chan:]))).astype(BF16)
            return jnp.dot(act, wo_v[l], preferred_element_type=F32)

        def update(c, k, mixed, first, last):
            new = bufs[c % 2][pl.ds(base[k], blk), :] + mixed[:, :chan]
            if last:
                hout_v[q, k] = new
            else:
                bufs[1 - c % 2][pl.ds(base[k], blk), :] = new
            skip_v[q, k] = mixed[:, chan:] if first else skip_v[q, k] + mixed[:, chan:]

        def layers(steps, layer_of, whole):
            pre, mixed = {}, {}
            for t in range(len(steps) + 2 * lag):
                if t < len(steps):
                    if whole and t == 0:
                        begin(0)
                    if whole and t + 1 < count:
                        begin(t + 1)
                    c, k = steps[t]
                    pre[t] = gates(layer_of(c), c % n_cyc, k)
                if 0 <= t - lag < len(steps):
                    mixed[t - lag] = activate(layer_of(steps[t - lag][0]), pre.pop(t - lag))
                if 0 <= t - 2 * lag:
                    c, k = steps[t - 2 * lag]
                    update(c % n_cyc, k, mixed.pop(t - 2 * lag), whole and c == 0, whole and c == n_layers - 1)

        if kind in UNROLLED:
            layers([(c, k) for c in range(n_layers) for k in range(count) if c < n_layers - 1 or k not in unused], lambda c: c, True)
        else:
            for k in range(count):
                begin(k)
                skip_v[q, k] = jnp.zeros((blk, chan), F32)

            def cycle(r, carry):
                layers([(c, k) for c in range(n_cyc) for k in range(count)], lambda c: r * n_cyc + c, False)
                return carry

            lax.fori_loop(0, n_layers // n_cyc, cycle, 0)
            for k in range(count):
                hout_v[q, k] = bufs[0][pl.ds(base[k], blk), :]

    def deliver(src, q):
        out = [(k, seq, b) for k, seq, b, counts in units(PLAN[src][q]) if counts]
        for k, seq, b in sorted(out, key=lambda u: ((src // 2) ^ (u[2] // 2) != 3, u[2] % 2 == 0, u)):
            for part, dst, recv in ((hout_v, h_out, h_recv), (skip_v, s_out, s_recv)):
                if b == src:
                    dst[seq] = part[q, k]
                else:
                    pltpu.make_async_remote_copy(
                        src_ref=part.at[q, k], dst_ref=dst.at[seq], send_sem=o_send, recv_sem=recv,
                        device_id=dev(b), device_id_type=MESH).start()

    def run(q, carry):
        for kind in KINDS:
            where = [(d, i) for d in range(N_DEV) for i, sweep in enumerate(PLAN[d]) if tuple(n for _, n, _ in sweep) == kind]
            hit = functools.reduce(jnp.logical_or, [jnp.logical_and(me == d, q == i) for d, i in where])

            @pl.when(hit)
            def _():
                compute(q, kind)

        for d in range(N_DEV):
            @on(d)
            def _():
                for i in range(len(PLAN[d])):
                    @pl.when(q == i)
                    def _():
                        deliver(d, i)
        return carry

    lax.fori_loop(0, N_SWEEP, run, 0)

    def drain(ref, sem, count):
        while count > 0:
            part = ref.at[pl.ds(0, min(count, n_seq))]
            pltpu.make_async_copy(part, part, sem).wait()
            count -= n_seq

    for d in range(N_DEV):
        @on(d)
        def _():
            drain(x_own, x_send, sum(target != d for _, _, target, _, _ in wanted[d]))
            results = [b for q in range(len(PLAN[d])) for _, _, b, counts in units(PLAN[d][q]) if counts]
            kept = results.count(d)
            drain(h_out, o_send, 2 * (len(results) - kept))
            drain(h_out, h_recv, n_seq - kept)
            drain(s_out, s_recv, n_seq - kept)


def to_hbm(h_vmem, s_vmem, h_hbm, s_hbm, sems):
    piece = h_vmem.shape[0] // PIECES
    copies = []
    for i in range(PIECES):
        rows = pl.ds(i * piece, piece)
        for j, (src, dst) in enumerate(((h_vmem, h_hbm), (s_vmem, s_hbm))):
            copies.append(pltpu.make_async_copy(src.at[rows], dst.at[rows], sems.at[j, i]))
    for copy in copies:
        copy.start()
    for copy in copies:
        copy.wait()


def solution(mesh):
    seq_spec = P("batch", SEQ_AXES, None)

    def local_stack(x_loc, w_f0, w_f1, w_g0, w_g1, w_res, w_skip):
        n_rep, n_cyc, chan = w_f0.shape[:3]
        n_layers = n_rep * n_cyc
        n_seq, blk, _ = x_loc.shape
        pad = 2 ** (n_cyc - 1)
        weights = [w.reshape(n_layers, chan, chan) for w in (w_f0, w_f1, w_g0, w_g1, w_res, w_skip)]
        any_spec = pl.BlockSpec(memory_space=pl.ANY)
        vmem_spec = pl.BlockSpec(memory_space=pltpu.VMEM)
        out = jax.ShapeDtypeStruct((n_seq, blk, chan), F32)
        vmem_out = pltpu.VMEM((n_seq, blk, chan), F32)
        state = [pltpu.VMEM((sum(pad + n * blk for n in kind), chan), F32) for kind in KINDS for _ in range(2)]
        landed = pl.pallas_call(
            functools.partial(kernel, n_layers, n_cyc, blk, pad),
            out_shape=(vmem_out, vmem_out),
            in_specs=[any_spec] * 7,
            out_specs=(vmem_spec, vmem_spec),
            scratch_shapes=[
                pltpu.VMEM((n_seq, blk, chan), BF16),
                pltpu.VMEM((N_SWEEP, 8, blk, chan), BF16),
                pltpu.VMEM((n_layers, 2 * chan, 2 * chan), BF16),
                pltpu.VMEM((n_layers, chan, 2 * chan), BF16),
                pltpu.VMEM((N_SWEEP, 8, blk, chan), F32),
                pltpu.VMEM((N_SWEEP, 8, blk, chan), F32),
                pltpu.SemaphoreType.DMA((6,)),
                pltpu.SemaphoreType.DMA,
                pltpu.SemaphoreType.DMA,
                pltpu.SemaphoreType.DMA((N_SWEEP,)),
                pltpu.SemaphoreType.DMA,
                pltpu.SemaphoreType.DMA,
                pltpu.SemaphoreType.DMA,
                *state,
            ],
            compiler_params=pltpu.CompilerParams(collective_id=0, has_side_effects=True, vmem_limit_bytes=44 * 2**20),
        )(*[pltpu.with_memory_space_constraint(v, pltpu.HBM) for v in (x_loc, *weights)])
        return pl.pallas_call(
            to_hbm,
            out_shape=(out, out),
            in_specs=[vmem_spec, vmem_spec],
            out_specs=(any_spec, any_spec),
            scratch_shapes=[pltpu.SemaphoreType.DMA((2, PIECES))],
            compiler_params=pltpu.CompilerParams(vmem_limit_bytes=2 * 2**20),
        )(*landed)

    return jax.shard_map(local_stack, mesh=mesh, in_specs=(seq_spec, P(), P(), P(), P(), P(), P()), out_specs=(seq_spec, seq_spec), check_vma=False)
```

```python
import functools

import jax
import jax.numpy as jnp
from jax import lax
from jax.experimental import pallas as pl
from jax.experimental.pallas import tpu as pltpu
from jax.sharding import PartitionSpec as P

MESH = pl.DeviceIdType.MESH
SEQ_AXES = ("seq_hi", "seq")
N_DEV = 8
PIECES = 4
LAG = 2
UNROLLED = ((8,), (6,), (4, 4))
F32 = jnp.float32
BF16 = jnp.bfloat16

PLAN = (
    (
        ((19, 2, (0, 1)), (4, 2, (0, 1)), (6, 2, (0, 1)), (21, 2, (0, 1)),),
        ((14, 6, (0, 1, 2, 3, 4, 5)),),
        ((23, 6, (0, 1, 4, 5)),),
        ((22, 4, (0, 1, 2, 3)), (16, 4, (0, 1, 2, 3)),),
        ((12, 2, (0, 1)), (3, 2, (0, 1)), (13, 2, (0, 1)), (11, 2, (0, 1)),),
    ),
    (
        ((15, 8, (0, 1, 4, 5, 6, 7)),),
        ((18, 8, (0, 1, 4, 5, 6, 7)),),
        ((20, 2, (0, 1)), (1, 2, (0, 1)), (8, 2, (0, 1)), (7, 2, (0, 1)),),
        ((10, 2, (0, 1)), (2, 2, (0, 1)), (0, 2, (0, 1)), (9, 2, (0, 1)),),
    ),
    (
        ((20, 4, (2, 3)), (10, 4, (2, 3)),),
        ((21, 8, (2, 3, 6, 7)),),
        ((23, 8, (2, 3, 6, 7)),),
        ((18, 4, (2, 3)), (9, 4, (2, 3)),),
    ),
    (
        ((13, 8, (2, 3, 4, 5, 6, 7)),),
        ((12, 8, (2, 3, 6, 7)),),
        ((5, 8, (0, 1, 2, 3, 4, 5, 6, 7)),),
        ((0, 4, (2, 3)), (17, 4, (2, 3)),),
        ((15, 4, (2, 3)), (3, 4, (2, 3)),),
    ),
    (
        ((22, 8, (4, 5, 6, 7)),),
        ((20, 8, (4, 5, 6, 7)),),
        ((3, 8, (4, 5, 6, 7)),),
        ((16, 8, (4, 5, 6, 7)),),
        ((12, 6, (4, 5)),),
    ),
    (
        ((10, 8, (4, 5, 6, 7)),),
        ((9, 8, (4, 5, 6, 7)),),
        ((17, 8, (0, 1, 4, 5, 6, 7)),),
        ((0, 8, (4, 5, 6, 7)),),
        ((21, 6, (4, 5)),),
    ),
    (
        ((8, 8, (2, 3, 4, 5, 6, 7)),),
        ((7, 8, (2, 3, 4, 5, 6, 7)),),
        ((2, 8, (2, 3, 4, 5, 6, 7)),),
        ((6, 8, (2, 3, 4, 5, 6, 7)),),
    ),
    (
        ((11, 8, (2, 3, 4, 5, 6, 7)),),
        ((4, 8, (2, 3, 4, 5, 6, 7)),),
        ((1, 8, (2, 3, 4, 5, 6, 7)),),
        ((19, 8, (2, 3, 4, 5, 6, 7)),),
        ((14, 8, (6, 7)),),
    ),
)
N_SWEEP = max(len(sweeps) for sweeps in PLAN)
KINDS = tuple(sorted({tuple(n for _, n, _ in sweep) for sweeps in PLAN for sweep in sweeps}, reverse=True))


def units(sweep):
    return [(k, *rest) for k, rest in enumerate((seq, b, b in keep) for seq, n, keep in sweep for b in range(n))]


def kernel(n_layers, n_cyc, blk, pad, x_ref, wf0, wf1, wg0, wg1, wr, ws, h_out, s_out,
           x_own, xbuf, wg_v, wo_v, hout_v, skip_v, w_sem, own_sem, x_send, x_recv, o_send, h_recv, s_recv, *state):
    me = lax.axis_index("seq_hi") * 4 + lax.axis_index("seq")
    chan = x_ref.shape[-1]
    n_seq = x_ref.shape[0]
    bufs_of = {kind: state[2 * i:2 * i + 2] for i, kind in enumerate(KINDS)}

    def dev(index):
        return {"seq_hi": index // 4, "seq": index % 4}

    def on(index):
        return pl.when(me == index)

    barrier = pltpu.get_barrier_semaphore()
    for step in range(1, N_DEV):
        other = lax.rem(me + step, N_DEV)
        pl.semaphore_signal(barrier, inc=1, device_id={"seq_hi": other // 4, "seq": lax.rem(other, 4)}, device_id_type=MESH)

    own = pltpu.make_async_copy(x_ref, x_own, own_sem)
    own.start()
    w_copies = [
        pltpu.make_async_copy(wf1, wg_v.at[:, pl.ds(0, chan), pl.ds(0, chan)], w_sem.at[0]),
        pltpu.make_async_copy(wg1, wg_v.at[:, pl.ds(0, chan), pl.ds(chan, chan)], w_sem.at[1]),
        pltpu.make_async_copy(wf0, wg_v.at[:, pl.ds(chan, chan), pl.ds(0, chan)], w_sem.at[2]),
        pltpu.make_async_copy(wg0, wg_v.at[:, pl.ds(chan, chan), pl.ds(chan, chan)], w_sem.at[3]),
        pltpu.make_async_copy(wr, wo_v.at[:, :, pl.ds(0, chan)], w_sem.at[4]),
        pltpu.make_async_copy(ws, wo_v.at[:, :, pl.ds(chan, chan)], w_sem.at[5]),
    ]
    for copy in w_copies:
        copy.start()

    pl.semaphore_wait(barrier, N_DEV - 1)
    own.wait()

    wanted = [[] for _ in range(N_DEV)]
    for target, sweeps in enumerate(PLAN):
        for q, sweep in enumerate(sweeps):
            for k, seq, b, _ in units(sweep):
                wanted[b].append((q, ((target // 2) ^ (b // 2) != 3, target % 2 == 0), target, k, seq))
    for src in range(N_DEV):
        @on(src)
        def _():
            for q, _, target, k, seq in sorted(wanted[src]):
                if target == src:
                    pltpu.make_async_copy(x_ref.at[seq], xbuf.at[q, k], x_recv.at[q]).start()
                else:
                    pltpu.make_async_remote_copy(
                        src_ref=x_own.at[seq], dst_ref=xbuf.at[q, k], send_sem=x_send, recv_sem=x_recv.at[q],
                        device_id=dev(target), device_id_type=MESH).start()

    for kind in KINDS:
        users = [d for d in range(N_DEV) if any(tuple(n for _, n, _ in sweep) == kind for sweep in PLAN[d])]
        uses = functools.reduce(jnp.logical_or, [me == d for d in users])

        @pl.when(uses)
        def _():
            first = 0
            for n in kind:
                for buf in bufs_of[kind]:
                    buf[pl.ds(first, pad), :] = jnp.zeros((pad, chan), F32)
                first += pad + n * blk

    for copy in w_copies:
        copy.wait()

    def halve(l, carry):
        wg_v[l, :, pl.ds(chan, chan)] = wg_v[l, :, pl.ds(chan, chan)] * BF16(0.5)
        wo_v[l] = wo_v[l] * BF16(0.5)
        return carry

    lax.fori_loop(0, n_layers, halve, 0)

    def compute(q, kind):
        bufs = bufs_of[kind]
        base, first = [], 0
        for n in kind:
            base += [first + pad + b * blk for b in range(n)]
            first += pad + n * blk
        count = len(base)
        everywhere = [units(sweep) for sweeps in PLAN for sweep in sweeps if tuple(n for _, n, _ in sweep) == kind]
        unused = [k for k in range(count) if not any(listed[k][3] for listed in everywhere)]
        lag = LAG if count > 4 else 1

        arrived = xbuf.at[q, pl.ds(0, count)]
        pltpu.make_async_copy(arrived, arrived, x_recv.at[q]).wait()

        def begin(k):
            bufs[0][pl.ds(base[k], blk), :] = xbuf[q, k].astype(F32)

        def gates(l, c, k):
            here = bufs[c % 2]
            lhs = jnp.concatenate([here[pl.ds(base[k], blk), :], here[pl.ds(base[k] - 2**c, blk), :]], axis=1).astype(BF16)
            return jnp.dot(lhs, wg_v[l], preferred_element_type=F32)

        def activate(l, pre):
            act = (jnp.tanh(pre[:, :chan]) * (1.0 + jnp.tanh(pre[:, chan:]))).astype(BF16)
            return jnp.dot(act, wo_v[l], preferred_element_type=F32)

        def update(c, k, mixed, first, last):
            new = bufs[c % 2][pl.ds(base[k], blk), :] + mixed[:, :chan]
            if last:
                hout_v[q, k] = new
            else:
                bufs[1 - c % 2][pl.ds(base[k], blk), :] = new
            skip_v[q, k] = mixed[:, chan:] if first else skip_v[q, k] + mixed[:, chan:]

        def layers(steps, layer_of, whole):
            pre, mixed = {}, {}
            for t in range(len(steps) + 2 * lag):
                if t < len(steps):
                    if whole and t == 0:
                        begin(0)
                    if whole and t + 1 < count:
                        begin(t + 1)
                    c, k = steps[t]
                    pre[t] = gates(layer_of(c), c % n_cyc, k)
                if 0 <= t - lag < len(steps):
                    mixed[t - lag] = activate(layer_of(steps[t - lag][0]), pre.pop(t - lag))
                if 0 <= t - 2 * lag:
                    c, k = steps[t - 2 * lag]
                    update(c % n_cyc, k, mixed.pop(t - 2 * lag), whole and c == 0, whole and c == n_layers - 1)

        if kind in UNROLLED:
            layers([(c, k) for c in range(n_layers) for k in range(count) if c < n_layers - 1 or k not in unused], lambda c: c, True)
        else:
            for k in range(count):
                begin(k)
                skip_v[q, k] = jnp.zeros((blk, chan), F32)

            def cycle(r, carry):
                layers([(c, k) for c in range(n_cyc) for k in range(count)], lambda c: r * n_cyc + c, False)
                return carry

            lax.fori_loop(0, n_layers // n_cyc, cycle, 0)
            for k in range(count):
                hout_v[q, k] = bufs[0][pl.ds(base[k], blk), :]

    def deliver(src, q):
        out = [(k, seq, b) for k, seq, b, counts in units(PLAN[src][q]) if counts]
        for k, seq, b in sorted(out, key=lambda u: ((src // 2) ^ (u[2] // 2) != 3, u[2] % 2 == 0, u)):
            for part, dst, recv in ((hout_v, h_out, h_recv), (skip_v, s_out, s_recv)):
                if b == src:
                    dst[seq] = part[q, k]
                else:
                    pltpu.make_async_remote_copy(
                        src_ref=part.at[q, k], dst_ref=dst.at[seq], send_sem=o_send, recv_sem=recv,
                        device_id=dev(b), device_id_type=MESH).start()

    def run(q, carry):
        for kind in KINDS:
            where = [(d, i) for d in range(N_DEV) for i, sweep in enumerate(PLAN[d]) if tuple(n for _, n, _ in sweep) == kind]
            hit = functools.reduce(jnp.logical_or, [jnp.logical_and(me == d, q == i) for d, i in where])

            @pl.when(hit)
            def _():
                compute(q, kind)

        for d in range(N_DEV):
            @on(d)
            def _():
                for i in range(len(PLAN[d])):
                    @pl.when(q == i)
                    def _():
                        deliver(d, i)
        return carry

    lax.fori_loop(0, N_SWEEP, run, 0)

    def drain(ref, sem, count):
        while count > 0:
            part = ref.at[pl.ds(0, min(count, n_seq))]
            pltpu.make_async_copy(part, part, sem).wait()
            count -= n_seq

    for d in range(N_DEV):
        @on(d)
        def _():
            drain(x_own, x_send, sum(target != d for _, _, target, _, _ in wanted[d]))
            results = [b for q in range(len(PLAN[d])) for _, _, b, counts in units(PLAN[d][q]) if counts]
            kept = results.count(d)
            drain(h_out, o_send, 2 * (len(results) - kept))
            drain(h_out, h_recv, n_seq - kept)
            drain(s_out, s_recv, n_seq - kept)


def to_hbm(h_vmem, s_vmem, h_hbm, s_hbm, sems):
    piece = h_vmem.shape[0] // PIECES
    copies = []
    for i in range(PIECES):
        rows = pl.ds(i * piece, piece)
        for j, (src, dst) in enumerate(((h_vmem, h_hbm), (s_vmem, s_hbm))):
            copies.append(pltpu.make_async_copy(src.at[rows], dst.at[rows], sems.at[j, i]))
    for copy in copies:
        copy.start()
    for copy in copies:
        copy.wait()


def solution(mesh):
    seq_spec = P("batch", SEQ_AXES, None)

    def local_stack(x_loc, w_f0, w_f1, w_g0, w_g1, w_res, w_skip):
        n_rep, n_cyc, chan = w_f0.shape[:3]
        n_layers = n_rep * n_cyc
        n_seq, blk, _ = x_loc.shape
        pad = 2 ** (n_cyc - 1)
        weights = [w.reshape(n_layers, chan, chan) for w in (w_f0, w_f1, w_g0, w_g1, w_res, w_skip)]
        any_spec = pl.BlockSpec(memory_space=pl.ANY)
        vmem_spec = pl.BlockSpec(memory_space=pltpu.VMEM)
        out = jax.ShapeDtypeStruct((n_seq, blk, chan), F32)
        vmem_out = pltpu.VMEM((n_seq, blk, chan), F32)
        state = [pltpu.VMEM((sum(pad + n * blk for n in kind), chan), F32) for kind in KINDS for _ in range(2)]
        landed = pl.pallas_call(
            functools.partial(kernel, n_layers, n_cyc, blk, pad),
            out_shape=(vmem_out, vmem_out),
            in_specs=[any_spec] * 7,
            out_specs=(vmem_spec, vmem_spec),
            scratch_shapes=[
                pltpu.VMEM((n_seq, blk, chan), BF16),
                pltpu.VMEM((N_SWEEP, 8, blk, chan), BF16),
                pltpu.VMEM((n_layers, 2 * chan, 2 * chan), BF16),
                pltpu.VMEM((n_layers, chan, 2 * chan), BF16),
                pltpu.VMEM((N_SWEEP, 8, blk, chan), F32),
                pltpu.VMEM((N_SWEEP, 8, blk, chan), F32),
                pltpu.SemaphoreType.DMA((6,)),
                pltpu.SemaphoreType.DMA,
                pltpu.SemaphoreType.DMA,
                pltpu.SemaphoreType.DMA((N_SWEEP,)),
                pltpu.SemaphoreType.DMA,
                pltpu.SemaphoreType.DMA,
                pltpu.SemaphoreType.DMA,
                *state,
            ],
            compiler_params=pltpu.CompilerParams(collective_id=0, has_side_effects=True, vmem_limit_bytes=44 * 2**20),
        )(*[pltpu.with_memory_space_constraint(v, pltpu.HBM) for v in (x_loc, *weights)])
        return pl.pallas_call(
            to_hbm,
            out_shape=(out, out),
            in_specs=[vmem_spec, vmem_spec],
            out_specs=(any_spec, any_spec),
            scratch_shapes=[pltpu.SemaphoreType.DMA((2, PIECES))],
            compiler_params=pltpu.CompilerParams(vmem_limit_bytes=2 * 2**20),
        )(*landed)

    return jax.shard_map(local_stack, mesh=mesh, in_specs=(seq_spec, P(), P(), P(), P(), P(), P()), out_specs=(seq_spec, seq_spec), check_vma=False)
```

```python
import functools

import jax
import jax.numpy as jnp
from jax import lax
from jax.experimental import pallas as pl
from jax.experimental.pallas import tpu as pltpu
from jax.sharding import PartitionSpec as P

MESH = pl.DeviceIdType.MESH
SEQ_AXES = ("seq_hi", "seq")
N_DEV = 8
PIECES = 4
LAG = 2
UNROLLED = ((8,), (6,), (4, 4))
F32 = jnp.float32
BF16 = jnp.bfloat16

PLAN = (
    (
        ((19, 2, (0, 1)), (4, 2, (0, 1)), (6, 2, (0, 1)), (21, 2, (0, 1)),),
        ((14, 6, (0, 1, 2, 3, 4, 5)),),
        ((23, 6, (0, 1, 4, 5)),),
        ((22, 4, (0, 1, 2, 3)), (16, 4, (0, 1, 2, 3)),),
        ((12, 2, (0, 1)), (3, 2, (0, 1)), (13, 2, (0, 1)), (11, 2, (0, 1)),),
    ),
    (
        ((15, 8, (0, 1, 4, 5, 6, 7)),),
        ((18, 8, (0, 1, 4, 5, 6, 7)),),
        ((20, 2, (0, 1)), (1, 2, (0, 1)), (8, 2, (0, 1)), (7, 2, (0, 1)),),
        ((10, 2, (0, 1)), (2, 2, (0, 1)), (0, 2, (0, 1)), (9, 2, (0, 1)),),
    ),
    (
        ((20, 4, (2, 3)), (10, 4, (2, 3)),),
        ((21, 8, (2, 3, 6, 7)),),
        ((23, 8, (2, 3, 6, 7)),),
        ((18, 4, (2, 3)), (9, 4, (2, 3)),),
    ),
    (
        ((13, 8, (2, 3, 4, 5, 6, 7)),),
        ((12, 8, (2, 3, 6, 7)),),
        ((5, 8, (0, 1, 2, 3, 4, 5, 6, 7)),),
        ((0, 4, (2, 3)), (17, 4, (2, 3)),),
        ((15, 4, (2, 3)), (3, 4, (2, 3)),),
    ),
    (
        ((22, 8, (4, 5, 6, 7)),),
        ((20, 8, (4, 5, 6, 7)),),
        ((3, 8, (4, 5, 6, 7)),),
        ((16, 8, (4, 5, 6, 7)),),
        ((12, 6, (4, 5)),),
    ),
    (
        ((10, 8, (4, 5, 6, 7)),),
        ((9, 8, (4, 5, 6, 7)),),
        ((17, 8, (0, 1, 4, 5, 6, 7)),),
        ((0, 8, (4, 5, 6, 7)),),
        ((21, 6, (4, 5)),),
    ),
    (
        ((8, 8, (2, 3, 4, 5, 6, 7)),),
        ((7, 8, (2, 3, 4, 5, 6, 7)),),
        ((2, 8, (2, 3, 4, 5, 6, 7)),),
        ((6, 8, (2, 3, 4, 5, 6, 7)),),
    ),
    (
        ((11, 8, (2, 3, 4, 5, 6, 7)),),
        ((4, 8, (2, 3, 4, 5, 6, 7)),),
        ((1, 8, (2, 3, 4, 5, 6, 7)),),
        ((19, 8, (2, 3, 4, 5, 6, 7)),),
        ((14, 8, (6, 7)),),
    ),
)
N_SWEEP = max(len(sweeps) for sweeps in PLAN)
KINDS = tuple(sorted({tuple(n for _, n, _ in sweep) for sweeps in PLAN for sweep in sweeps}, reverse=True))


def units(sweep):
    return [(k, *rest) for k, rest in enumerate((seq, b, b in keep) for seq, n, keep in sweep for b in range(n))]


def kernel(n_layers, n_cyc, blk, pad, x_ref, wf0, wf1, wg0, wg1, wr, ws, h_out, s_out,
           x_own, xbuf, wg_v, wo_v, hout_v, skip_v, w_sem, own_sem, x_send, x_recv, o_send, h_recv, s_recv, *state):
    me = lax.axis_index("seq_hi") * 4 + lax.axis_index("seq")
    chan = x_ref.shape[-1]
    n_seq = x_ref.shape[0]
    bufs_of = {kind: state[2 * i:2 * i + 2] for i, kind in enumerate(KINDS)}

    def dev(index):
        return {"seq_hi": index // 4, "seq": index % 4}

    def on(index):
        return pl.when(me == index)

    barrier = pltpu.get_barrier_semaphore()
    for step in range(1, N_DEV):
        other = lax.rem(me + step, N_DEV)
        pl.semaphore_signal(barrier, inc=1, device_id={"seq_hi": other // 4, "seq": lax.rem(other, 4)}, device_id_type=MESH)

    own = pltpu.make_async_copy(x_ref, x_own, own_sem)
    own.start()
    w_copies = [
        pltpu.make_async_copy(wf1, wg_v.at[:, pl.ds(0, chan), pl.ds(0, chan)], w_sem.at[0]),
        pltpu.make_async_copy(wg1, wg_v.at[:, pl.ds(0, chan), pl.ds(chan, chan)], w_sem.at[1]),
        pltpu.make_async_copy(wf0, wg_v.at[:, pl.ds(chan, chan), pl.ds(0, chan)], w_sem.at[2]),
        pltpu.make_async_copy(wg0, wg_v.at[:, pl.ds(chan, chan), pl.ds(chan, chan)], w_sem.at[3]),
        pltpu.make_async_copy(wr, wo_v.at[:, :, pl.ds(0, chan)], w_sem.at[4]),
        pltpu.make_async_copy(ws, wo_v.at[:, :, pl.ds(chan, chan)], w_sem.at[5]),
    ]
    for copy in w_copies:
        copy.start()

    pl.semaphore_wait(barrier, N_DEV - 1)
    own.wait()

    wanted = [[] for _ in range(N_DEV)]
    for target, sweeps in enumerate(PLAN):
        for q, sweep in enumerate(sweeps):
            for k, seq, b, _ in units(sweep):
                wanted[b].append((q, ((target // 2) ^ (b // 2) != 3, (target % 2 == 0) != (target // 2 == 2)), target, k, seq))
    for src in range(N_DEV):
        @on(src)
        def _():
            for q, _, target, k, seq in sorted(wanted[src]):
                if target == src:
                    pltpu.make_async_copy(x_ref.at[seq], xbuf.at[q, k], x_recv.at[q]).start()
                else:
                    pltpu.make_async_remote_copy(
                        src_ref=x_own.at[seq], dst_ref=xbuf.at[q, k], send_sem=x_send, recv_sem=x_recv.at[q],
                        device_id=dev(target), device_id_type=MESH).start()

    for kind in KINDS:
        users = [d for d in range(N_DEV) if any(tuple(n for _, n, _ in sweep) == kind for sweep in PLAN[d])]
        uses = functools.reduce(jnp.logical_or, [me == d for d in users])

        @pl.when(uses)
        def _():
            first = 0
            for n in kind:
                for buf in bufs_of[kind]:
                    buf[pl.ds(first, pad), :] = jnp.zeros((pad, chan), F32)
                first += pad + n * blk

    for copy in w_copies:
        copy.wait()

    def halve(l, carry):
        wg_v[l, :, pl.ds(chan, chan)] = wg_v[l, :, pl.ds(chan, chan)] * BF16(0.5)
        wo_v[l] = wo_v[l] * BF16(0.5)
        return carry

    lax.fori_loop(0, n_layers, halve, 0)

    def compute(q, kind):
        bufs = bufs_of[kind]
        base, first = [], 0
        for n in kind:
            base += [first + pad + b * blk for b in range(n)]
            first += pad + n * blk
        count = len(base)
        everywhere = [units(sweep) for sweeps in PLAN for sweep in sweeps if tuple(n for _, n, _ in sweep) == kind]
        unused = [k for k in range(count) if not any(listed[k][3] for listed in everywhere)]
        lag = LAG if count > 4 else 1

        arrived = xbuf.at[q, pl.ds(0, count)]
        pltpu.make_async_copy(arrived, arrived, x_recv.at[q]).wait()

        def begin(k):
            bufs[0][pl.ds(base[k], blk), :] = xbuf[q, k].astype(F32)

        def gates(l, c, k):
            here = bufs[c % 2]
            lhs = jnp.concatenate([here[pl.ds(base[k], blk), :], here[pl.ds(base[k] - 2**c, blk), :]], axis=1).astype(BF16)
            return jnp.dot(lhs, wg_v[l], preferred_element_type=F32)

        def activate(l, pre):
            act = (jnp.tanh(pre[:, :chan]) * (1.0 + jnp.tanh(pre[:, chan:]))).astype(BF16)
            return jnp.dot(act, wo_v[l], preferred_element_type=F32)

        def update(c, k, mixed, first, last):
            new = bufs[c % 2][pl.ds(base[k], blk), :] + mixed[:, :chan]
            if last:
                hout_v[q, k] = new
            else:
                bufs[1 - c % 2][pl.ds(base[k], blk), :] = new
            skip_v[q, k] = mixed[:, chan:] if first else skip_v[q, k] + mixed[:, chan:]

        def layers(steps, layer_of, whole):
            pre, mixed = {}, {}
            for t in range(len(steps) + 2 * lag):
                if t < len(steps):
                    if whole and t == 0:
                        begin(0)
                    if whole and t + 1 < count:
                        begin(t + 1)
                    c, k = steps[t]
                    pre[t] = gates(layer_of(c), c % n_cyc, k)
                if 0 <= t - lag < len(steps):
                    mixed[t - lag] = activate(layer_of(steps[t - lag][0]), pre.pop(t - lag))
                if 0 <= t - 2 * lag:
                    c, k = steps[t - 2 * lag]
                    update(c % n_cyc, k, mixed.pop(t - 2 * lag), whole and c == 0, whole and c == n_layers - 1)

        if kind in UNROLLED:
            layers([(c, k) for c in range(n_layers) for k in range(count) if c < n_layers - 1 or k not in unused], lambda c: c, True)
        else:
            for k in range(count):
                begin(k)
                skip_v[q, k] = jnp.zeros((blk, chan), F32)

            def cycle(r, carry):
                layers([(c, k) for c in range(n_cyc) for k in range(count)], lambda c: r * n_cyc + c, False)
                return carry

            lax.fori_loop(0, n_layers // n_cyc, cycle, 0)
            for k in range(count):
                hout_v[q, k] = bufs[0][pl.ds(base[k], blk), :]

    def deliver(src, q):
        out = [(k, seq, b) for k, seq, b, counts in units(PLAN[src][q]) if counts]
        for k, seq, b in sorted(out, key=lambda u: ((src // 2) ^ (u[2] // 2) != 3, u[2] % 2 == 0, u)):
            for part, dst, recv in ((hout_v, h_out, h_recv), (skip_v, s_out, s_recv)):
                if b == src:
                    dst[seq] = part[q, k]
                else:
                    pltpu.make_async_remote_copy(
                        src_ref=part.at[q, k], dst_ref=dst.at[seq], send_sem=o_send, recv_sem=recv,
                        device_id=dev(b), device_id_type=MESH).start()

    def run(q, carry):
        for kind in KINDS:
            where = [(d, i) for d in range(N_DEV) for i, sweep in enumerate(PLAN[d]) if tuple(n for _, n, _ in sweep) == kind]
            hit = functools.reduce(jnp.logical_or, [jnp.logical_and(me == d, q == i) for d, i in where])

            @pl.when(hit)
            def _():
                compute(q, kind)

        for d in range(N_DEV):
            @on(d)
            def _():
                for i in range(len(PLAN[d])):
                    @pl.when(q == i)
                    def _():
                        deliver(d, i)
        return carry

    lax.fori_loop(0, N_SWEEP, run, 0)

    def drain(ref, sem, count):
        while count > 0:
            part = ref.at[pl.ds(0, min(count, n_seq))]
            pltpu.make_async_copy(part, part, sem).wait()
            count -= n_seq

    for d in range(N_DEV):
        @on(d)
        def _():
            drain(x_own, x_send, sum(target != d for _, _, target, _, _ in wanted[d]))
            results = [b for q in range(len(PLAN[d])) for _, _, b, counts in units(PLAN[d][q]) if counts]
            kept = results.count(d)
            drain(h_out, o_send, 2 * (len(results) - kept))
            drain(h_out, h_recv, n_seq - kept)
            drain(s_out, s_recv, n_seq - kept)


def to_hbm(h_vmem, s_vmem, h_hbm, s_hbm, sems):
    piece = h_vmem.shape[0] // PIECES
    copies = []
    for i in range(PIECES):
        rows = pl.ds(i * piece, piece)
        for j, (src, dst) in enumerate(((h_vmem, h_hbm), (s_vmem, s_hbm))):
            copies.append(pltpu.make_async_copy(src.at[rows], dst.at[rows], sems.at[j, i]))
    for copy in copies:
        copy.start()
    for copy in copies:
        copy.wait()


def solution(mesh):
    seq_spec = P("batch", SEQ_AXES, None)

    def local_stack(x_loc, w_f0, w_f1, w_g0, w_g1, w_res, w_skip):
        n_rep, n_cyc, chan = w_f0.shape[:3]
        n_layers = n_rep * n_cyc
        n_seq, blk, _ = x_loc.shape
        pad = 2 ** (n_cyc - 1)
        weights = [w.reshape(n_layers, chan, chan) for w in (w_f0, w_f1, w_g0, w_g1, w_res, w_skip)]
        any_spec = pl.BlockSpec(memory_space=pl.ANY)
        vmem_spec = pl.BlockSpec(memory_space=pltpu.VMEM)
        out = jax.ShapeDtypeStruct((n_seq, blk, chan), F32)
        vmem_out = pltpu.VMEM((n_seq, blk, chan), F32)
        state = [pltpu.VMEM((sum(pad + n * blk for n in kind), chan), F32) for kind in KINDS for _ in range(2)]
        landed = pl.pallas_call(
            functools.partial(kernel, n_layers, n_cyc, blk, pad),
            out_shape=(vmem_out, vmem_out),
            in_specs=[any_spec] * 7,
            out_specs=(vmem_spec, vmem_spec),
            scratch_shapes=[
                pltpu.VMEM((n_seq, blk, chan), BF16),
                pltpu.VMEM((N_SWEEP, 8, blk, chan), BF16),
                pltpu.VMEM((n_layers, 2 * chan, 2 * chan), BF16),
                pltpu.VMEM((n_layers, chan, 2 * chan), BF16),
                pltpu.VMEM((N_SWEEP, 8, blk, chan), F32),
                pltpu.VMEM((N_SWEEP, 8, blk, chan), F32),
                pltpu.SemaphoreType.DMA((6,)),
                pltpu.SemaphoreType.DMA,
                pltpu.SemaphoreType.DMA,
                pltpu.SemaphoreType.DMA((N_SWEEP,)),
                pltpu.SemaphoreType.DMA,
                pltpu.SemaphoreType.DMA,
                pltpu.SemaphoreType.DMA,
                *state,
            ],
            compiler_params=pltpu.CompilerParams(collective_id=0, has_side_effects=True, vmem_limit_bytes=44 * 2**20),
        )(*[pltpu.with_memory_space_constraint(v, pltpu.HBM) for v in (x_loc, *weights)])
        return pl.pallas_call(
            to_hbm,
            out_shape=(out, out),
            in_specs=[vmem_spec, vmem_spec],
            out_specs=(any_spec, any_spec),
            scratch_shapes=[pltpu.SemaphoreType.DMA((2, PIECES))],
            compiler_params=pltpu.CompilerParams(vmem_limit_bytes=2 * 2**20),
        )(*landed)

    return jax.shard_map(local_stack, mesh=mesh, in_specs=(seq_spec, P(), P(), P(), P(), P(), P()), out_specs=(seq_spec, seq_spec), check_vma=False)
```

```python
import functools

import jax
import jax.numpy as jnp
from jax import lax
from jax.experimental import pallas as pl
from jax.experimental.pallas import tpu as pltpu
from jax.sharding import PartitionSpec as P

MESH = pl.DeviceIdType.MESH
SEQ_AXES = ("seq_hi", "seq")
N_DEV = 8
PIECES = 8
LAG = 2
UNROLLED = ((8,), (6,), (4, 4))
F32 = jnp.float32
BF16 = jnp.bfloat16

PLAN = (
    (
        ((19, 2, (0, 1)), (4, 2, (0, 1)), (6, 2, (0, 1)), (21, 2, (0, 1)),),
        ((14, 6, (0, 1, 2, 3, 4, 5)),),
        ((23, 6, (0, 1, 4, 5)),),
        ((22, 4, (0, 1, 2, 3)), (16, 4, (0, 1, 2, 3)),),
        ((12, 2, (0, 1)), (3, 2, (0, 1)), (13, 2, (0, 1)), (11, 2, (0, 1)),),
    ),
    (
        ((15, 8, (0, 1, 4, 5, 6, 7)),),
        ((18, 8, (0, 1, 4, 5, 6, 7)),),
        ((20, 2, (0, 1)), (1, 2, (0, 1)), (8, 2, (0, 1)), (7, 2, (0, 1)),),
        ((10, 2, (0, 1)), (2, 2, (0, 1)), (0, 2, (0, 1)), (9, 2, (0, 1)),),
    ),
    (
        ((20, 4, (2, 3)), (10, 4, (2, 3)),),
        ((21, 8, (2, 3, 6, 7)),),
        ((23, 8, (2, 3, 6, 7)),),
        ((18, 4, (2, 3)), (9, 4, (2, 3)),),
    ),
    (
        ((13, 8, (2, 3, 4, 5, 6, 7)),),
        ((12, 8, (2, 3, 6, 7)),),
        ((5, 8, (0, 1, 2, 3, 4, 5, 6, 7)),),
        ((0, 4, (2, 3)), (17, 4, (2, 3)),),
        ((15, 4, (2, 3)), (3, 4, (2, 3)),),
    ),
    (
        ((22, 8, (4, 5, 6, 7)),),
        ((20, 8, (4, 5, 6, 7)),),
        ((3, 8, (4, 5, 6, 7)),),
        ((16, 8, (4, 5, 6, 7)),),
        ((12, 6, (4, 5)),),
    ),
    (
        ((10, 8, (4, 5, 6, 7)),),
        ((9, 8, (4, 5, 6, 7)),),
        ((17, 8, (0, 1, 4, 5, 6, 7)),),
        ((0, 8, (4, 5, 6, 7)),),
        ((21, 6, (4, 5)),),
    ),
    (
        ((8, 8, (2, 3, 4, 5, 6, 7)),),
        ((7, 8, (2, 3, 4, 5, 6, 7)),),
        ((2, 8, (2, 3, 4, 5, 6, 7)),),
        ((6, 8, (2, 3, 4, 5, 6, 7)),),
    ),
    (
        ((11, 8, (2, 3, 4, 5, 6, 7)),),
        ((4, 8, (2, 3, 4, 5, 6, 7)),),
        ((1, 8, (2, 3, 4, 5, 6, 7)),),
        ((19, 8, (2, 3, 4, 5, 6, 7)),),
        ((14, 8, (6, 7)),),
    ),
)
N_SWEEP = max(len(sweeps) for sweeps in PLAN)
KINDS = tuple(sorted({tuple(n for _, n, _ in sweep) for sweeps in PLAN for sweep in sweeps}, reverse=True))


def units(sweep):
    return [(k, *rest) for k, rest in enumerate((seq, b, b in keep) for seq, n, keep in sweep for b in range(n))]


def kernel(n_layers, n_cyc, blk, pad, x_ref, wf0, wf1, wg0, wg1, wr, ws, h_out, s_out,
           x_own, xbuf, wg_v, wo_v, hout_v, skip_v, w_sem, own_sem, x_send, x_recv, o_send, h_recv, s_recv, *state):
    me = lax.axis_index("seq_hi") * 4 + lax.axis_index("seq")
    chan = x_ref.shape[-1]
    n_seq = x_ref.shape[0]
    bufs_of = {kind: state[2 * i:2 * i + 2] for i, kind in enumerate(KINDS)}

    def dev(index):
        return {"seq_hi": index // 4, "seq": index % 4}

    def on(index):
        return pl.when(me == index)

    barrier = pltpu.get_barrier_semaphore()
    for step in range(1, N_DEV):
        other = lax.rem(me + step, N_DEV)
        pl.semaphore_signal(barrier, inc=1, device_id={"seq_hi": other // 4, "seq": lax.rem(other, 4)}, device_id_type=MESH)

    own = pltpu.make_async_copy(x_ref, x_own, own_sem)
    own.start()
    w_copies = [
        pltpu.make_async_copy(wf1, wg_v.at[:, pl.ds(0, chan), pl.ds(0, chan)], w_sem.at[0]),
        pltpu.make_async_copy(wg1, wg_v.at[:, pl.ds(0, chan), pl.ds(chan, chan)], w_sem.at[1]),
        pltpu.make_async_copy(wf0, wg_v.at[:, pl.ds(chan, chan), pl.ds(0, chan)], w_sem.at[2]),
        pltpu.make_async_copy(wg0, wg_v.at[:, pl.ds(chan, chan), pl.ds(chan, chan)], w_sem.at[3]),
        pltpu.make_async_copy(wr, wo_v.at[:, :, pl.ds(0, chan)], w_sem.at[4]),
        pltpu.make_async_copy(ws, wo_v.at[:, :, pl.ds(chan, chan)], w_sem.at[5]),
    ]
    for copy in w_copies:
        copy.start()

    pl.semaphore_wait(barrier, N_DEV - 1)
    own.wait()

    wanted = [[] for _ in range(N_DEV)]
    for target, sweeps in enumerate(PLAN):
        for q, sweep in enumerate(sweeps):
            for k, seq, b, _ in units(sweep):
                wanted[b].append((q, ((target // 2) ^ (b // 2) != 3, (target % 2 == 0) != (target // 2 == 2)), target, k, seq))
    for src in range(N_DEV):
        @on(src)
        def _():
            for q, _, target, k, seq in sorted(wanted[src]):
                if target == src:
                    pltpu.make_async_copy(x_ref.at[seq], xbuf.at[q, k], x_recv.at[q]).start()
                else:
                    pltpu.make_async_remote_copy(
                        src_ref=x_own.at[seq], dst_ref=xbuf.at[q, k], send_sem=x_send, recv_sem=x_recv.at[q],
                        device_id=dev(target), device_id_type=MESH).start()

    for kind in KINDS:
        users = [d for d in range(N_DEV) if any(tuple(n for _, n, _ in sweep) == kind for sweep in PLAN[d])]
        uses = functools.reduce(jnp.logical_or, [me == d for d in users])

        @pl.when(uses)
        def _():
            first = 0
            for n in kind:
                for buf in bufs_of[kind]:
                    buf[pl.ds(first, pad), :] = jnp.zeros((pad, chan), F32)
                first += pad + n * blk

    for copy in w_copies:
        copy.wait()

    def halve(l, carry):
        wg_v[l, :, pl.ds(chan, chan)] = wg_v[l, :, pl.ds(chan, chan)] * BF16(0.5)
        wo_v[l] = wo_v[l] * BF16(0.5)
        return carry

    lax.fori_loop(0, n_layers, halve, 0)

    def compute(q, kind):
        bufs = bufs_of[kind]
        base, first = [], 0
        for n in kind:
            base += [first + pad + b * blk for b in range(n)]
            first += pad + n * blk
        count = len(base)
        everywhere = [units(sweep) for sweeps in PLAN for sweep in sweeps if tuple(n for _, n, _ in sweep) == kind]
        unused = [k for k in range(count) if not any(listed[k][3] for listed in everywhere)]
        lag = LAG if count > 4 else 1

        arrived = xbuf.at[q, pl.ds(0, count)]
        pltpu.make_async_copy(arrived, arrived, x_recv.at[q]).wait()

        def begin(k):
            bufs[0][pl.ds(base[k], blk), :] = xbuf[q, k].astype(F32)

        def gates(l, c, k):
            here = bufs[c % 2]
            lhs = jnp.concatenate([here[pl.ds(base[k], blk), :], here[pl.ds(base[k] - 2**c, blk), :]], axis=1).astype(BF16)
            return jnp.dot(lhs, wg_v[l], preferred_element_type=F32)

        def activate(l, pre):
            act = (jnp.tanh(pre[:, :chan]) * (1.0 + jnp.tanh(pre[:, chan:]))).astype(BF16)
            return jnp.dot(act, wo_v[l], preferred_element_type=F32)

        def update(c, k, mixed, first, last):
            new = bufs[c % 2][pl.ds(base[k], blk), :] + mixed[:, :chan]
            if last:
                hout_v[q, k] = new
            else:
                bufs[1 - c % 2][pl.ds(base[k], blk), :] = new
            skip_v[q, k] = mixed[:, chan:] if first else skip_v[q, k] + mixed[:, chan:]

        def layers(steps, layer_of, whole):
            pre, mixed = {}, {}
            for t in range(len(steps) + 2 * lag):
                if t < len(steps):
                    if whole and t == 0:
                        begin(0)
                    if whole and t + 1 < count:
                        begin(t + 1)
                    c, k = steps[t]
                    pre[t] = gates(layer_of(c), c % n_cyc, k)
                if 0 <= t - lag < len(steps):
                    mixed[t - lag] = activate(layer_of(steps[t - lag][0]), pre.pop(t - lag))
                if 0 <= t - 2 * lag:
                    c, k = steps[t - 2 * lag]
                    update(c % n_cyc, k, mixed.pop(t - 2 * lag), whole and c == 0, whole and c == n_layers - 1)

        if kind in UNROLLED:
            layers([(c, k) for c in range(n_layers) for k in range(count) if c < n_layers - 1 or k not in unused], lambda c: c, True)
        else:
            for k in range(count):
                begin(k)
                skip_v[q, k] = jnp.zeros((blk, chan), F32)

            def cycle(r, carry):
                layers([(c, k) for c in range(n_cyc) for k in range(count)], lambda c: r * n_cyc + c, False)
                return carry

            lax.fori_loop(0, n_layers // n_cyc, cycle, 0)
            for k in range(count):
                hout_v[q, k] = bufs[0][pl.ds(base[k], blk), :]

    def deliver(src, q):
        out = [(k, seq, b) for k, seq, b, counts in units(PLAN[src][q]) if counts]
        for k, seq, b in sorted(out, key=lambda u: ((src // 2) ^ (u[2] // 2) != 3, u[2] % 2 == 0, u)):
            for part, dst, recv in ((hout_v, h_out, h_recv), (skip_v, s_out, s_recv)):
                if b == src:
                    dst[seq] = part[q, k]
                else:
                    pltpu.make_async_remote_copy(
                        src_ref=part.at[q, k], dst_ref=dst.at[seq], send_sem=o_send, recv_sem=recv,
                        device_id=dev(b), device_id_type=MESH).start()

    def run(q, carry):
        for kind in KINDS:
            where = [(d, i) for d in range(N_DEV) for i, sweep in enumerate(PLAN[d]) if tuple(n for _, n, _ in sweep) == kind]
            hit = functools.reduce(jnp.logical_or, [jnp.logical_and(me == d, q == i) for d, i in where])

            @pl.when(hit)
            def _():
                compute(q, kind)

        for d in range(N_DEV):
            @on(d)
            def _():
                for i in range(len(PLAN[d])):
                    @pl.when(q == i)
                    def _():
                        deliver(d, i)
        return carry

    lax.fori_loop(0, N_SWEEP, run, 0)

    def drain(ref, sem, count):
        while count > 0:
            part = ref.at[pl.ds(0, min(count, n_seq))]
            pltpu.make_async_copy(part, part, sem).wait()
            count -= n_seq

    for d in range(N_DEV):
        @on(d)
        def _():
            drain(x_own, x_send, sum(target != d for _, _, target, _, _ in wanted[d]))
            results = [b for q in range(len(PLAN[d])) for _, _, b, counts in units(PLAN[d][q]) if counts]
            kept = results.count(d)
            drain(h_out, o_send, 2 * (len(results) - kept))
            drain(h_out, h_recv, n_seq - kept)
            drain(s_out, s_recv, n_seq - kept)


def to_hbm(h_vmem, s_vmem, h_hbm, s_hbm, sems):
    piece = h_vmem.shape[0] // PIECES
    copies = []
    for i in range(PIECES):
        rows = pl.ds(i * piece, piece)
        for j, (src, dst) in enumerate(((h_vmem, h_hbm), (s_vmem, s_hbm))):
            copies.append(pltpu.make_async_copy(src.at[rows], dst.at[rows], sems.at[j, i]))
    for copy in copies:
        copy.start()
    for copy in copies:
        copy.wait()


def solution(mesh):
    seq_spec = P("batch", SEQ_AXES, None)

    def local_stack(x_loc, w_f0, w_f1, w_g0, w_g1, w_res, w_skip):
        n_rep, n_cyc, chan = w_f0.shape[:3]
        n_layers = n_rep * n_cyc
        n_seq, blk, _ = x_loc.shape
        pad = 2 ** (n_cyc - 1)
        weights = [w.reshape(n_layers, chan, chan) for w in (w_f0, w_f1, w_g0, w_g1, w_res, w_skip)]
        any_spec = pl.BlockSpec(memory_space=pl.ANY)
        vmem_spec = pl.BlockSpec(memory_space=pltpu.VMEM)
        out = jax.ShapeDtypeStruct((n_seq, blk, chan), F32)
        vmem_out = pltpu.VMEM((n_seq, blk, chan), F32)
        state = [pltpu.VMEM((sum(pad + n * blk for n in kind), chan), F32) for kind in KINDS for _ in range(2)]
        landed = pl.pallas_call(
            functools.partial(kernel, n_layers, n_cyc, blk, pad),
            out_shape=(vmem_out, vmem_out),
            in_specs=[any_spec] * 7,
            out_specs=(vmem_spec, vmem_spec),
            scratch_shapes=[
                pltpu.VMEM((n_seq, blk, chan), BF16),
                pltpu.VMEM((N_SWEEP, 8, blk, chan), BF16),
                pltpu.VMEM((n_layers, 2 * chan, 2 * chan), BF16),
                pltpu.VMEM((n_layers, chan, 2 * chan), BF16),
                pltpu.VMEM((N_SWEEP, 8, blk, chan), F32),
                pltpu.VMEM((N_SWEEP, 8, blk, chan), F32),
                pltpu.SemaphoreType.DMA((6,)),
                pltpu.SemaphoreType.DMA,
                pltpu.SemaphoreType.DMA,
                pltpu.SemaphoreType.DMA((N_SWEEP,)),
                pltpu.SemaphoreType.DMA,
                pltpu.SemaphoreType.DMA,
                pltpu.SemaphoreType.DMA,
                *state,
            ],
            compiler_params=pltpu.CompilerParams(collective_id=0, has_side_effects=True, vmem_limit_bytes=44 * 2**20),
        )(*[pltpu.with_memory_space_constraint(v, pltpu.HBM) for v in (x_loc, *weights)])
        return pl.pallas_call(
            to_hbm,
            out_shape=(out, out),
            in_specs=[vmem_spec, vmem_spec],
            out_specs=(any_spec, any_spec),
            scratch_shapes=[pltpu.SemaphoreType.DMA((2, PIECES))],
            compiler_params=pltpu.CompilerParams(vmem_limit_bytes=2 * 2**20),
        )(*landed)

    return jax.shard_map(local_stack, mesh=mesh, in_specs=(seq_spec, P(), P(), P(), P(), P(), P()), out_specs=(seq_spec, seq_spec), check_vma=False)
```
